32 devices in a mesh: row: 8 (over z, x), mem: 2 (over core), lev: 2 (over y).
Axes of the slice: x: 2, y: 2, z: 4, core: 2. Of those that a mesh axis runs over, the one named last changes fastest.
Arguments:
- control_fields: bfloat16 [4, 6, 256, 2048], P('mem', 'lev', 'row'), may hold values from -6 to 6
- perturbations: bfloat16 [3, 4, 6, 256, 2048], P(None, 'mem', 'lev', 'row'), may hold values from -3 to 3
- column_taper: bfloat16 [2048, 2048], P('row'), may hold values from -1 to 2, as said below
- row_taper: bfloat16 [256, 256], P('row'), may hold values from -1 to 2, as said below
- courant_numbers: float32 [3, 6, 256, 2048], P(None, 'lev', 'row', 'mem'), may hold values from -0.3 to 0.3
- tracer_slope: float32 [2, 6, 256, 2048], P(None, 'lev', 'row', 'mem'), may hold values from -3 to 3
Outputs:
- increment: float32 [3, 6, 256, 2048], P(None, 'lev', 'row', 'mem')
The draws below stay inside these ranges and needn't reach their ends.
Inputs may be any that keep to these rules, and one draw needn't show every extreme that they name: `column_taper`: A square matrix. `row_taper`: A square matrix.
All inputs are finite; a program needn't handle non-finite values.
Results may differ from the reference program's by a relative error of at most 0.0048.
Values may be sent and summed in bfloat16 or wider, within the bound.
A program may use at most 64 MiB of HBM per device.

```python
import jax
import jax.numpy as jnp
from jax import lax

NX = 2048
STEPS = 4
NY = 256
M = 4
LEV = 6


def banded(key, order):
    first_index = jnp.arange(order)[:, None]
    second_index = jnp.arange(order)[None, :]
    reach = order / 4.0
    noise = jnp.clip(jax.random.normal(key, (order, order), jnp.float32), -4.0, 4.0)
    distance = jnp.abs(first_index - second_index).astype(jnp.float32)
    diagonal = jnp.where(first_index == second_index, 1.0, 0.0).astype(jnp.float32)
    return (diagonal + noise * jnp.exp(-distance / reach) / jnp.sqrt(reach)).astype(jnp.bfloat16)


def draw_column_taper(key, part):
    return banded(jax.random.fold_in(key, 11), NX)


def draw_row_taper(key, part):
    return banded(jax.random.fold_in(key, 23), NY)


def level_of(own_key, shape, pieces, low, top_value):
    gain = 1.0
    for axis_at, parts in pieces:
        heights = jax.random.uniform(jax.random.fold_in(jax.random.fold_in(own_key, 6), axis_at), (parts,), jnp.float32, low / len(pieces), top_value / len(pieces))
        gain = gain * jnp.repeat(jnp.exp(heights), shape[axis_at] // parts).reshape((-1,) + (1,) * (len(shape) - 1 - axis_at))
    return gain


def scatter_about(own_key, dims, width, bound, split=(), held_as=jnp.bfloat16):
    array = jax.random.normal(own_key, dims, jnp.float32) * width
    if len(split) > 0:
        array = level_of(own_key, dims, split, -0.22, 0.18) * array
    return jnp.clip(array, min=-bound, max=bound).astype(held_as)


def setup_inputs(seed: int = 0) -> dict:
    key_list = jax.random.split(jax.random.key(seed), 7)
    return {
        "control_fields": scatter_about(key_list[0], (M, LEV, NY, NX), 1.0, 6.0, ((0, 2), (1, 2), (2, 8))),
        "perturbations": scatter_about(key_list[1], (3, M, LEV, NY, NX), M ** -0.5, 3.0, ((1, 2), (2, 2), (3, 8))),
        "column_taper": draw_column_taper(jax.random.fold_in(key_list[6], 71), 0),
        "row_taper": draw_row_taper(jax.random.fold_in(key_list[6], 71), 0),
        "courant_numbers": jnp.clip(jax.random.uniform(key_list[4], (3, LEV, NY, NX), jnp.float32, -0.3, 0.3) * level_of(key_list[4], (3, LEV, NY, NX), ((1, 2), (2, 8), (3, 2)), -0.4, 0.0), -0.3, 0.3),
        "tracer_slope": scatter_about(key_list[5], (2, LEV, NY, NX), 0.5, 3.0, ((1, 2), (2, 8), (3, 2)), jnp.float32),
    }


def upwind(middle, behind, forward, velocity):
    return jnp.maximum(velocity, 0.0) * (middle - behind) + jnp.minimum(velocity, 0.0) * (forward - middle)


def advance(present, courant_numbers, tracer_slope, padded):
    middle = padded[:, 1:-1, 1:-1, 1:-1]
    change = upwind(middle, padded[:, :-2, 1:-1, 1:-1], padded[:, 2:, 1:-1, 1:-1], courant_numbers[0])
    change = change + upwind(middle, padded[:, 1:-1, :-2, 1:-1], padded[:, 1:-1, 2:, 1:-1], courant_numbers[1])
    change = change + upwind(middle, padded[:, 1:-1, 1:-1, :-2], padded[:, 1:-1, 1:-1, 2:], courant_numbers[2])
    shifted = present - change
    source = present[0] * tracer_slope[0] + present[1] * tracer_slope[1]
    return jnp.concatenate([shifted[:2], shifted[2:] - source[None]], axis=0)


def reference(control_fields, perturbations, column_taper, row_taper, courant_numbers, tracer_slope):
    def per_level(plane):
        first_pass = jnp.dot(plane, column_taper, preferred_element_type=jnp.float32).astype(jnp.bfloat16)
        return jnp.dot(row_taper, first_pass, preferred_element_type=jnp.float32).astype(jnp.bfloat16)

    def accumulate(running, member_pair):
        control_one, perturb_one = member_pair
        localized = lax.map(per_level, control_one)
        return running + perturb_one.astype(jnp.float32) * localized.astype(jnp.float32)[None], None

    starting = jnp.zeros((3,) + control_fields.shape[1:], jnp.float32)
    present, ignored = lax.scan(accumulate, starting, (control_fields, jnp.moveaxis(perturbations, 1, 0)))
    for advect_step in range(STEPS):
        padded = jnp.pad(present, ((0, 0), (1, 1), (1, 1), (1, 1)))
        present = advance(present, courant_numbers, tracer_slope, padded)
    return present
```

```python
import jax
import jax.numpy as jnp
from jax import lax
from jax.experimental import pallas as pl
from jax.experimental.pallas import tpu as pltpu
from jax.sharding import PartitionSpec as P

STEPS = 4


MESH = pl.DeviceIdType.MESH
AXES = ("lev", "row", "mem")


def sides():
    found = []
    for at, axis in enumerate(AXES):
        here, count = lax.axis_index(axis), lax.axis_size(axis)
        if count > 1:
            found.append((at, 0, axis, here > 0, here - 1))
            found.append((at, 1, axis, here < count - 1, here + 1))
    return found


def advect_kernel(
    first, courant, slope, out, state, factors, level_send, row_send, level_halo, row_halo,
    column_halo, send_sem, recv_sem,
):
    kinds, levels, rows, width = first.shape
    barrier = pltpu.get_barrier_semaphore()
    neighbours = sides()
    for at, side, axis, there, target in neighbours:

        @pl.when(there)
        def _():
            pl.semaphore_signal(barrier, inc=1, device_id={axis: target}, device_id_type=MESH)

    row_at = lax.broadcasted_iota(jnp.int32, (rows, width), 0)
    column_at = lax.broadcasted_iota(jnp.int32, (rows, width), 1)
    for level in range(levels):
        centre = jnp.ones((rows, width), jnp.float32)
        for at in range(3):
            ahead = jnp.maximum(courant[at, level], 0.0)
            back = jnp.minimum(courant[at, level], 0.0)
            centre = centre - ahead + back
            if at == 1:
                ahead = jnp.where(row_at == 0, 0.0, ahead)
                back = jnp.where(row_at == rows - 1, 0.0, back)
            if at == 2:
                ahead = jnp.where(column_at == 0, 0.0, ahead)
                back = jnp.where(column_at == width - 1, 0.0, back)
            factors[1 + 2 * at, level] = ahead
            factors[2 + 2 * at, level] = back
        factors[0, level] = centre
    for kind in range(kinds):
        for level in range(levels):
            state[0, kind, level] = first[kind, level]
    pl.semaphore_wait(barrier, sum(there.astype(jnp.int32) for _, _, _, there, _ in neighbours))

    def copy_of(step, at, side, axis, target):
        if at == 0:
            source, landing = level_send.at[step, side], level_halo.at[step, 1 - side]
        elif at == 1:
            source, landing = row_send.at[step, side], row_halo.at[step, 1 - side]
        else:
            lanes = pl.ds(0 if side == 0 else width - 128, 128)
            source = state.at[step, :, :, :, lanes]
            landing = column_halo.at[step, 1 - side]
        return pltpu.make_async_remote_copy(
            src_ref=source,
            dst_ref=landing,
            send_sem=send_sem.at[step, 2 * at + side],
            recv_sem=recv_sem.at[step, 2 * at + 1 - side],
            device_id={axis: target},
            device_id_type=MESH,
        )

    def arrival(step, at, side, axis, target):
        landing = (level_halo, row_halo, column_halo)[at].at[step, side]
        return pltpu.make_async_remote_copy(
            src_ref=landing,
            dst_ref=landing,
            send_sem=send_sem.at[step, 2 * at + side],
            recv_sem=recv_sem.at[step, 2 * at + side],
            device_id={axis: target},
            device_id_type=MESH,
        )

    def one_step(step, target_ref):
        for at, side, axis, there, target in neighbours:

            @pl.when(there)
            def _():
                for kind in range(kinds):
                    if at == 0:
                        level_send[step, side, kind] = state[
                            step, kind, 0 if side == 0 else levels - 1
                        ].astype(level_send.dtype)
                    if at == 1:
                        edge = 0 if side == 0 else rows - 1
                        for level in range(levels):
                            row_send[step, side, pl.ds(kind * levels + level, 1)] = state[
                                step, kind, level, pl.ds(edge, 1)
                            ]
                copy_of(step, at, side, axis, target).start()

        for level in range(levels):
            for kind in range(kinds):
                here = state[step, kind, level]
                new = here * factors[0, level]
                new = new + factors[3, level] * pltpu.roll(here, 1, 0)
                new = new - factors[4, level] * pltpu.roll(here, rows - 1, 0)
                new = new + factors[5, level] * pltpu.roll(here, 1, 1)
                new = new - factors[6, level] * pltpu.roll(here, width - 1, 1)
                if level > 0:
                    new = new + factors[1, level] * state[step, kind, level - 1]
                if level < levels - 1:
                    new = new - factors[2, level] * state[step, kind, level + 1]
                if kind == 2:
                    new = new - (
                        state[step, 0, level] * slope[0, level]
                        + state[step, 1, level] * slope[1, level]
                    )
                target_ref[kind, level] = new

        lane_at = lax.broadcasted_iota(jnp.int32, (rows, 128), 1)
        for at, side, axis, there, target in (
            [n for n in neighbours if n[0] == 2]
            + [n for n in neighbours if n[0] == 1]
            + [n for n in neighbours if n[0] == 0]
        ):

            @pl.when(there)
            def _():
                arrival(step, at, side, axis, target).wait_recv()
                for kind in range(kinds):
                    if at == 0:
                        level = 0 if side == 0 else levels - 1
                        term = factors[1 + side, level] * level_halo[step, side, kind].astype(
                            jnp.float32
                        )
                        if side:
                            term = -term
                        target_ref[kind, level] = target_ref[kind, level] + term
                        continue
                    for level in range(levels):
                        if at == 1:
                            edge = pl.ds(0 if side == 0 else rows - 1, 1)
                            speed = courant[1, level, edge]
                            speed = jnp.minimum(speed, 0.0) if side else jnp.maximum(speed, 0.0)
                            term = speed * row_halo[step, side, pl.ds(kind * levels + level, 1)]
                            if side:
                                term = -term
                            target_ref[kind, level, edge] = target_ref[kind, level, edge] + term
                        else:
                            lanes = pl.ds(width - 128 if side else 0, 128)
                            speed = courant[2, level, :, lanes]
                            speed = jnp.minimum(speed, 0.0) if side else jnp.maximum(speed, 0.0)
                            beside = pltpu.roll(
                                column_halo[step, side, kind, level], 127 if side else 1, 1
                            )
                            term = jnp.where(
                                lane_at == (127 if side else 0), speed * beside, 0.0
                            )
                            if side:
                                term = -term
                            target_ref[kind, level, :, lanes] = (
                                target_ref[kind, level, :, lanes] + term
                            )

    @pl.loop(0, STEPS - 1)
    def _(step):
        one_step(step, state.at[step + 1])

    one_step(STEPS - 1, out)

    @pl.loop(0, STEPS)
    def _(step):
        for at, side, axis, there, target in neighbours:

            @pl.when(there)
            def _():
                copy_of(step, at, side, axis, target).wait_send()


def advected(weighted, courant_numbers, tracer_slope):
    kinds, levels, rows, width = weighted.shape
    edges = -(-kinds * levels // 8) * 8
    return pl.pallas_call(
        advect_kernel,
        out_shape=jax.ShapeDtypeStruct(weighted.shape, jnp.float32),
        in_specs=[pl.BlockSpec(memory_space=pltpu.VMEM)] * 3,
        out_specs=pl.BlockSpec(memory_space=pltpu.VMEM),
        scratch_shapes=[
            pltpu.VMEM((STEPS, kinds, levels, rows, width), jnp.float32),
            pltpu.VMEM((7, levels, rows, width), jnp.float32),
            pltpu.VMEM((STEPS, 2, kinds, rows, width), jnp.bfloat16),
            pltpu.VMEM((STEPS, 2, edges, width), jnp.float32),
            pltpu.VMEM((STEPS, 2, kinds, rows, width), jnp.bfloat16),
            pltpu.VMEM((STEPS, 2, edges, width), jnp.float32),
            pltpu.VMEM((STEPS, 2, kinds, levels, rows, 128), jnp.float32),
            pltpu.SemaphoreType.DMA((STEPS, 6)),
            pltpu.SemaphoreType.DMA((STEPS, 6)),
        ],
        compiler_params=pltpu.CompilerParams(
            collective_id=1, has_side_effects=True, vmem_limit_bytes=48 << 20
        ),
        name="advect",
    )(weighted, courant_numbers, tracer_slope)


def localize_kernel(
    control, pert, taper, row_part, out, own, gathered, row_all, staged, halves, taper_all, pert_all,
    one_send, one_recv, row_send, row_recv, two_send, two_recv, pass_send, pass_recv, pert_send,
    pert_recv, first_send, first_recv, line_send, line_recv, side_send, side_recv, lev_send, lev_recv,
    own_sem,
):
    count, mems, levs = (lax.axis_size(axis) for axis in ("row", "mem", "lev"))
    me, mem_at, lev_at = (lax.axis_index(axis) for axis in ("row", "mem", "lev"))
    kinds, members, levels, rows, columns = pert.shape
    depth, width = taper.shape[0], out.shape[3]
    inner = 2 if count % 2 == 0 else 1
    outer = count // inner
    line_at, side_at = me // inner, me % inner
    share, lanes = depth // levs, width // inner
    sent = []

    def remote(source, landing, to, at, **target):
        return pltpu.make_async_remote_copy(
            src_ref=source, dst_ref=landing, send_sem=to, recv_sem=at, device_id=target,
            device_id_type=MESH,
        )

    def send(there, copy):
        sent.append((there, copy))
        when(there, lambda: copy().start())

    def when(there, action):
        if there is True:
            action()
        else:
            pl.when(there)(action)

    def own_columns(at):
        return pl.ds(pl.multiple_of(at * width, width), width)

    def block(source, at, level):
        if len(source.shape) == 5:
            return source.at[at, :, level]
        return source.at[:, level, :, pl.ds(pl.multiple_of(at * depth, depth), depth)]

    def level_of(turn):
        return jnp.where(lev_at > 0, turn, levels - 1 - turn)

    offsets = sorted(range(1, count), key=lambda by: -min(by // inner, outer - by // inner))

    def peer_of(by):
        return (line_at + by // inner) % outer * inner + (side_at + by % inner) % inner

    def one(peer, slot, level):
        return remote(
            block(own, peer, level), gathered.at[slot, level], one_send.at[peer, level],
            one_recv.at[slot, level], row=peer,
        )

    def row(peer, slot):
        return remote(row_all.at[me], row_all.at[slot], row_send.at[peer], row_recv.at[slot], row=peer)

    def two(peer, slot, level):
        return remote(
            staged.at[peer, level], halves.at[level, slot, mem_at], two_send.at[peer, level],
            two_recv.at[slot, level], row=peer,
        )

    def onward(peer, slot, level, place):
        part = halves.at[level, slot, place]
        return remote(
            part, part, pass_send.at[peer, slot, level], pass_recv.at[place, slot, level], mem=peer
        )

    def pert_copy(peer, slot):
        return remote(
            pert.at[:, :, :, :, own_columns(peer)], pert_all.at[slot], pert_send.at[peer],
            pert_recv.at[slot], mem=peer,
        )

    def piece(origin, lev, side):
        return taper_all.at[
            origin,
            pl.ds(pl.multiple_of(lev * share, share), share),
            pl.ds(pl.multiple_of(side * lanes, lanes), lanes),
        ]

    other = line_at * inner + (inner - 1 - side_at)

    def first(origin, side):
        part = piece(origin, lev_at, side)
        return remote(part, part, first_send.at[0], first_recv.at[0], row=other)

    def side(origin, at):
        part = piece(origin, lev_at, at)
        return remote(part, part, side_send.at[origin], side_recv.at[origin], row=other)

    def line(way, hop, turn, sending):
        back = hop if sending else hop + 1
        from_line = line_at - back if way == 0 else line_at + back
        to_line = line_at + 1 if way == 0 else line_at - 1
        origin = from_line * inner + (side_at if turn == 0 else inner - 1 - side_at)
        there = from_line >= 0 if way == 0 else from_line <= outer - 1
        if sending:
            there = there & (to_line <= outer - 1 if way == 0 else to_line >= 0)

        def copy():
            part = piece(origin, lev_at, side_at)
            return remote(
                part, part, line_send.at[way, hop, turn], line_recv.at[way, hop, turn],
                row=to_line * inner + side_at,
            )

        return origin, there, copy

    def lev_copy(origin, at, shift, sending):
        part = piece(origin, lev_at if sending else (lev_at + levs - shift) % levs, at)
        return remote(
            part, part, lev_send.at[origin, at, shift - 1], lev_recv.at[origin, at, shift - 1],
            lev=(lev_at + shift) % levs,
        )

    def across(there, origin, at):
        for shift in range(1, levs):
            send(there, lambda shift=shift: lev_copy(origin, at, shift, True))

    def along_line(hop, turn):
        if outer == 1:
            return
        for way in range(2):
            _, there, copy = line(way, hop, turn, True)
            send(there, copy)

    def one_chunk(turn):
        level = level_of(turn)
        for by in offsets:
            send(True, lambda by=by: one(peer_of(by), me, level))

    def row_step(turn):
        level = level_of(turn)
        for by in offsets:
            slot = peer_of(by)
            one(slot, slot, level).wait_recv()
        whole = row_all[...].reshape(count * rows, count * rows)
        for member in range(members):
            tapered = jnp.dot(
                whole, gathered[:, level, member].reshape(count * rows, depth),
                preferred_element_type=jnp.float32,
            )
            staged[:, level, member] = tapered.astype(jnp.bfloat16).reshape(count, rows, depth)
        for by in offsets:
            send(True, lambda by=by: two(peer_of(by), me, level))
        for member in range(members):
            halves[level, me, mem_at, member] = staged[me, level, member]
        for shift in range(1, mems):
            send(True, lambda shift=shift: onward((mem_at + shift) % mems, me, level, mem_at))

    barrier = pltpu.get_barrier_semaphore()
    for axis, here, size in (("row", me, count), ("mem", mem_at, mems), ("lev", lev_at, levs)):

        @pl.loop(1, size)
        def _(shift):
            pl.semaphore_signal(
                barrier, inc=1, device_id={axis: (here + shift) % size}, device_id_type=MESH
            )

    fetches = [
        pltpu.make_async_copy(taper.at[:, own_columns(mem_at)], taper_all.at[me], own_sem.at[0]),
        pltpu.make_async_copy(control, own, own_sem.at[1]),
        pltpu.make_async_copy(row_part, row_all.at[me], own_sem.at[2]),
        pltpu.make_async_copy(
            pert.at[:, :, :, :, own_columns(mem_at)], pert_all.at[mem_at], own_sem.at[3]
        ),
    ]
    for level in range(levels):
        fetches.append(
            pltpu.make_async_copy(
                block(control, me, level), gathered.at[me, level], own_sem.at[4 + level]
            )
        )
    for fetch in fetches:
        fetch.start()
    for fetch in fetches[:3]:
        fetch.wait()
    pl.semaphore_wait(barrier, count + mems + levs - 3)

    if inner > 1:
        send(True, lambda: first(me, inner - 1 - side_at))
    along_line(0, 0)
    if inner > 1:
        send(True, lambda: side(me, side_at))
    for by in offsets:
        send(True, lambda by=by: row(peer_of(by), me))
    one_chunk(0)
    for shift in range(1, mems):
        send(True, lambda shift=shift: pert_copy((mem_at + shift) % mems, mem_at))
    for fetch in fetches[3:]:
        fetch.wait()
    if inner > 1:
        first(other, side_at).wait_recv()
        along_line(0, 1)
        across(True, other, side_at)
    for turn in range(1, levels - 1):
        one_chunk(turn)
    if inner > 1:
        side(other, inner - 1 - side_at).wait_recv()
        across(True, other, inner - 1 - side_at)

    def hop_step(hop):
        for turn in range(inner):
            for way in range(2):
                origin, there, copy = line(way, hop, turn, False)

                def arrived(copy=copy):
                    copy().wait_recv()

                when(there, arrived)
                if hop + 1 < outer - 1:
                    _, onwards, relay = line(way, hop + 1, turn, True)
                    send(onwards, relay)
                if inner > 1:
                    send(there, lambda origin=origin: side(origin, side_at))
                across(there, origin, side_at)

    def side_step(hop):
        for turn in range(inner):
            for way in range(2):
                origin, there, _ = line(way, hop, turn, False)
                if inner > 1:

                    def arrived(origin=origin):
                        side(origin, inner - 1 - side_at).wait_recv()

                    when(there, arrived)
                    across(there, origin, inner - 1 - side_at)

    ready = 0
    for hop in range(outer - 1):
        hop_step(hop)
        if hop == 0:
            one_chunk(levels - 1)
            for by in offsets:
                slot = peer_of(by)
                row(slot, slot).wait_recv()
        if ready < levels:
            row_step(ready)
            ready += 1
        side_step(hop)
    for turn in range(ready, levels):
        row_step(turn)

    for turn in range(levels):
        level = level_of(turn)
        for by in offsets:
            slot = peer_of(by)
            two(slot, slot, level).wait_recv()
            for shift in range(1, mems):
                send(
                    True,
                    lambda shift=shift, slot=slot, level=level: onward(
                        (mem_at + shift) % mems, slot, level, mem_at
                    ),
                )

    for by in offsets:
        origin = peer_of(by)
        for at in range(inner):
            for shift in range(1, levs):
                lev_copy(origin, at, shift, False).wait_recv()
    for shift in range(1, mems):
        peer = (mem_at + shift) % mems
        pert_copy(peer, peer).wait_recv()

    span = min(width, 256)
    for turn in range(levels):
        level = level_of(turn)
        for shift in range(1, mems):
            peer = (mem_at + shift) % mems

            @pl.loop(0, count)
            def _(slot):
                onward(peer, slot, level, peer).wait_recv()

        for start in range(0, width, span):
            total = jnp.zeros((mems * members * rows, span), jnp.float32)
            for slot in range(count):
                total = total + jnp.dot(
                    halves[level, slot].reshape(mems * members * rows, depth),
                    taper_all[slot, :, pl.ds(start, span)],
                    preferred_element_type=jnp.float32,
                )
            for kind in range(kinds):
                weighted = jnp.zeros((rows, span), jnp.float32)
                for mem in range(mems):
                    for member in range(members):
                        at = (mem * members + member) * rows
                        weighted = weighted + pert_all[
                            mem, kind, member, level, :, pl.ds(start, span)
                        ].astype(jnp.float32) * total[at : at + rows]
                out[kind, level, :, pl.ds(start, span)] = weighted

    for there, copy in sent:
        when(there, lambda copy=copy: copy().wait_send())


def localized(control_fields, perturbations, column_taper, row_taper):
    members, levels, rows, columns = control_fields.shape
    kinds = perturbations.shape[0]
    count, mems, levs = (lax.axis_size(axis) for axis in ("row", "mem", "lev"))
    depth, width = columns // count, columns // mems
    if depth % 128:
        control_fields = control_fields.reshape(members, levels, rows, count, depth)
        control_fields = control_fields.transpose(3, 0, 1, 2, 4)
    low, dma = jnp.bfloat16, pltpu.SemaphoreType.DMA
    pairs = [dma((count, levels))] * 2 + [dma((count,))] * 2 + [dma((count, levels))] * 2
    pairs += [dma((mems, count, levels))] * 2 + [dma((mems,))] * 2 + [dma((1,))] * 2
    pairs += [dma((2, count, 2))] * 2 + [dma((count,))] * 2 + [dma((count, 2, levs))] * 2
    return pl.pallas_call(
        localize_kernel,
        out_shape=jax.ShapeDtypeStruct((kinds, levels, rows, width), jnp.float32),
        in_specs=[pl.BlockSpec(memory_space=pl.ANY)] * 4,
        out_specs=pl.BlockSpec(memory_space=pltpu.VMEM),
        scratch_shapes=[
            pltpu.VMEM(control_fields.shape, low),
            pltpu.VMEM((count, levels, members, rows, depth), low),
            pltpu.VMEM((count, rows, count * rows), low),
            pltpu.VMEM((count, levels, members, rows, depth), low),
            pltpu.VMEM((levels, count, mems, members, rows, depth), low),
            pltpu.VMEM((count, depth, width), low),
            pltpu.VMEM((mems, kinds, members, levels, rows, width), low),
            *pairs,
            dma((4 + levels,)),
        ],
        compiler_params=pltpu.CompilerParams(
            collective_id=0, has_side_effects=True, vmem_limit_bytes=56 << 20
        ),
        name="localize",
    )(control_fields, perturbations, column_taper, row_taper)


def on_device(
    control_fields, perturbations, column_taper, row_taper, courant_numbers, tracer_slope
):
    weighted = localized(control_fields, perturbations, column_taper, row_taper)
    return advected(weighted, courant_numbers, tracer_slope)


def solution(mesh):
    placed = (
        P("mem", "lev", "row", None),
        P(None, "mem", "lev", "row", None),
        P("row", None),
        P("row", None),
        P(None, "lev", "row", "mem"),
        P(None, "lev", "row", "mem"),
    )
    return jax.shard_map(
        on_device,
        mesh=mesh,
        in_specs=placed,
        out_specs=P(None, "lev", "row", "mem"),
        check_vma=False,
    )
```

```python
import jax
import jax.numpy as jnp
from jax import lax
from jax.experimental import pallas as pl
from jax.experimental.pallas import tpu as pltpu
from jax.sharding import PartitionSpec as P

STEPS = 4


MESH = pl.DeviceIdType.MESH


def kernel(
    control, pert, taper, row_part, courant_in, slope_in, out, own, gathered, row_all, staged, halves,
    taper_all, pert_all, courant, slope, state, factors, level_send, level_halo, row_edge, row_halo,
    column_halo, one_send, one_recv, row_send, row_recv, two_send, two_recv, pass_send, pass_recv,
    pert_send, pert_recv, first_send, first_recv, line_send, line_recv, side_send, side_recv, lev_send,
    lev_recv, up_send, up_recv, edge_send, edge_recv, column_send, column_recv, own_sem,
):
    count, mems, levs = (lax.axis_size(axis) for axis in ("row", "mem", "lev"))
    me, mem_at, lev_at = (lax.axis_index(axis) for axis in ("row", "mem", "lev"))
    kinds, members, levels, rows, columns = pert.shape
    depth, width = taper.shape[0], out.shape[3]
    inner = 2 if count % 2 == 0 else 1
    outer = count // inner
    line_at, side_at = me // inner, me % inner
    share, lanes = depth // levs, width // inner
    sent = []

    def remote(source, landing, to, at, **target):
        return pltpu.make_async_remote_copy(
            src_ref=source, dst_ref=landing, send_sem=to, recv_sem=at, device_id=target,
            device_id_type=MESH,
        )

    def send(there, copy):
        sent.append((there, copy))
        when(there, lambda: copy().start())

    def when(there, action):
        if there is True:
            action()
        else:
            pl.when(there)(action)

    def own_columns(at):
        return pl.ds(pl.multiple_of(at * width, width), width)

    def block(source, at, level):
        if len(source.shape) == 5:
            return source.at[at, :, level]
        return source.at[:, level, :, pl.ds(pl.multiple_of(at * depth, depth), depth)]

    def level_of(turn):
        return jnp.where(lev_at > 0, turn, levels - 1 - turn)

    offsets = sorted(range(1, count), key=lambda by: -min(by // inner, outer - by // inner))

    def peer_of(by):
        return (line_at + by // inner) % outer * inner + (side_at + by % inner) % inner

    def one(peer, slot, level):
        return remote(
            block(own, peer, level), gathered.at[slot, level], one_send.at[peer, level],
            one_recv.at[slot, level], row=peer,
        )

    def row(peer, slot):
        return remote(row_all.at[me], row_all.at[slot], row_send.at[peer], row_recv.at[slot], row=peer)

    def two(peer, slot, level):
        return remote(
            staged.at[peer, level], halves.at[level, slot, mem_at], two_send.at[peer, level],
            two_recv.at[slot, level], row=peer,
        )

    def onward(peer, slot, level, place):
        part = halves.at[level, slot, place]
        return remote(
            part, part, pass_send.at[peer, slot, level], pass_recv.at[place, slot, level], mem=peer
        )

    def pert_copy(peer, slot):
        return remote(
            pert.at[:, :, :, :, own_columns(peer)], pert_all.at[slot], pert_send.at[peer],
            pert_recv.at[slot], mem=peer,
        )

    def piece(origin, lev, side):
        return taper_all.at[
            origin,
            pl.ds(pl.multiple_of(lev * share, share), share),
            pl.ds(pl.multiple_of(side * lanes, lanes), lanes),
        ]

    other = line_at * inner + (inner - 1 - side_at)

    def first(origin, side):
        part = piece(origin, lev_at, side)
        return remote(part, part, first_send.at[0], first_recv.at[0], row=other)

    def side(origin, at):
        part = piece(origin, lev_at, at)
        return remote(part, part, side_send.at[origin], side_recv.at[origin], row=other)

    def line(way, hop, turn, sending):
        back = hop if sending else hop + 1
        from_line = line_at - back if way == 0 else line_at + back
        to_line = line_at + 1 if way == 0 else line_at - 1
        origin = from_line * inner + (side_at if turn == 0 else inner - 1 - side_at)
        there = from_line >= 0 if way == 0 else from_line <= outer - 1
        if sending:
            there = there & (to_line <= outer - 1 if way == 0 else to_line >= 0)

        def copy():
            part = piece(origin, lev_at, side_at)
            return remote(
                part, part, line_send.at[way, hop, turn], line_recv.at[way, hop, turn],
                row=to_line * inner + side_at,
            )

        return origin, there, copy

    def lev_copy(origin, at, shift, sending):
        part = piece(origin, lev_at if sending else (lev_at + levs - shift) % levs, at)
        return remote(
            part, part, lev_send.at[origin, at, shift - 1], lev_recv.at[origin, at, shift - 1],
            lev=(lev_at + shift) % levs,
        )

    def across(there, origin, at):
        for shift in range(1, levs):
            send(there, lambda shift=shift: lev_copy(origin, at, shift, True))

    def along_line(hop, turn):
        if outer == 1:
            return
        for way in range(2):
            _, there, copy = line(way, hop, turn, True)
            send(there, copy)

    def one_chunk(turn):
        level = level_of(turn)
        for by in offsets:
            send(True, lambda by=by: one(peer_of(by), me, level))

    def row_step(turn):
        level = level_of(turn)
        for by in offsets:
            slot = peer_of(by)
            one(slot, slot, level).wait_recv()
        whole = row_all[...].reshape(count * rows, count * rows)
        for member in range(members):
            tapered = jnp.dot(
                whole, gathered[:, level, member].reshape(count * rows, depth),
                preferred_element_type=jnp.float32,
            )
            staged[:, level, member] = tapered.astype(jnp.bfloat16).reshape(count, rows, depth)
        for by in offsets:
            send(True, lambda by=by: two(peer_of(by), me, level))
        for member in range(members):
            halves[level, me, mem_at, member] = staged[me, level, member]
        for shift in range(1, mems):
            send(True, lambda shift=shift: onward((mem_at + shift) % mems, me, level, mem_at))

    def set_factors():
        row_at = lax.broadcasted_iota(jnp.int32, (rows, width), 0)
        column_at = lax.broadcasted_iota(jnp.int32, (rows, width), 1)
        for turn in range(levels):
            level = level_of(turn)
            centre = jnp.ones((rows, width), jnp.float32)
            for at in range(3):
                speed = courant[at, level]
                ahead, back = jnp.maximum(speed, 0.0), -jnp.minimum(speed, 0.0)
                centre = centre - ahead - back
                if at == 0:
                    ahead, back = jnp.where(lev_at > 0, ahead, back), jnp.where(lev_at > 0, back, ahead)
                if at == 1:
                    ahead = jnp.where(row_at == 0, 0.0, ahead)
                    back = jnp.where(row_at == rows - 1, 0.0, back)
                if at == 2:
                    ahead = jnp.where(column_at == 0, 0.0, ahead)
                    back = jnp.where(column_at == width - 1, 0.0, back)
                factors[1 + 2 * at, turn] = ahead
                factors[2 + 2 * at, turn] = back
            factors[0, turn] = centre

    neighbours = []
    if count > 1:
        neighbours += [("row", 0, me > 0, me - 1), ("row", 1, me < count - 1, me + 1)]
    if mems > 1:
        neighbours += [("mem", 0, mem_at > 0, mem_at - 1), ("mem", 1, mem_at < mems - 1, mem_at + 1)]

    def part_of(turn):
        return min(turn, 1)

    def turns_of(part):
        return range(0, 1) if part == 0 else range(1, levels)

    parts = 1 if levels == 1 else 2

    def edge_copy(step, kind, part, axis, at, target, arriving):
        turns = pl.ds(0, 1) if part == 0 else pl.ds(1, levels - 1)
        landed = at if arriving else 1 - at
        if axis == "row":
            source = row_edge.at[step, at, kind, turns]
            landing = row_halo.at[step, landed, kind, turns]
            to, there = edge_send.at[step, at, kind, part], edge_recv.at[step, landed, kind, part]
        else:
            source = state.at[step, kind, turns, :, pl.ds(0 if at == 0 else width - 128, 128)]
            landing = column_halo.at[step, landed, kind, turns]
            to, there = column_send.at[step, at, kind, part], column_recv.at[step, landed, kind, part]
        return remote(landing if arriving else source, landing, to, there, **{axis: target})

    def level_copy(step, kind):
        return remote(
            level_send.at[step, kind], level_halo.at[step, kind], up_send.at[step, kind],
            up_recv.at[step, kind], lev=levs - 1 - lev_at,
        )

    def send_edges(step, kind, part):
        for axis, at, there, target in neighbours:

            @pl.when(there)
            def _():
                if axis == "row":
                    for turn in turns_of(part):
                        row_edge[step, at, kind, turn] = state[
                            step, kind, turn, pl.ds(0 if at == 0 else rows - 1, 1)
                        ]
                edge_copy(step, kind, part, axis, at, target, False).start()

    def inside(step, kind, turn, target):
        here = state[step, kind, turn]
        new = here * factors[0, turn]
        new = new + factors[3, turn] * pltpu.roll(here, 1, 0)
        new = new + factors[4, turn] * pltpu.roll(here, rows - 1, 0)
        new = new + factors[5, turn] * pltpu.roll(here, 1, 1)
        new = new + factors[6, turn] * pltpu.roll(here, width - 1, 1)
        if turn > 0:
            new = new + factors[1, turn] * state[step, kind, turn - 1]
        if turn < levels - 1:
            new = new + factors[2, turn] * state[step, kind, turn + 1]
        if kind == 2:
            level = level_of(turn)
            new = new - (
                state[step, 0, turn] * slope[0, level] + state[step, 1, turn] * slope[1, level]
            )
        target[...] = new

    def take_edges(step, kind, part, view):
        lane_at = lax.broadcasted_iota(jnp.int32, (rows, 128), 1)
        for axis, at, there, target in neighbours:

            @pl.when(there)
            def _():
                edge_copy(step, kind, part, axis, at, target, True).wait_recv()
                for turn in turns_of(part):
                    level, new = level_of(turn), view(kind, turn)
                    if axis == "row":
                        edge = pl.ds(0 if at == 0 else rows - 1, 1)
                        speed = courant[1, level, edge]
                        speed = -jnp.minimum(speed, 0.0) if at else jnp.maximum(speed, 0.0)
                        new[edge] = new[edge] + speed * row_halo[step, at, kind, turn]
                    else:
                        columns_at = pl.ds(width - 128 if at else 0, 128)
                        speed = courant[2, level, :, columns_at]
                        speed = -jnp.minimum(speed, 0.0) if at else jnp.maximum(speed, 0.0)
                        beside = pltpu.roll(column_halo[step, at, kind, turn], 127 if at else 1, 1)
                        new[:, columns_at] = new[:, columns_at] + jnp.where(
                            lane_at == (127 if at else 0), speed * beside, 0.0
                        )

    def one_step(step, view, last):
        for kind in range(kinds):
            inside(step, kind, 0, view(kind, 0))
            take_edges(step, kind, 0, view)
            if levs > 1:
                level_copy(step, kind).wait_recv()
                new = view(kind, 0)
                whole = new[...] + factors[1, 0] * level_halo[step, kind].astype(jnp.float32)
                new[...] = whole
                if not last:
                    level_send[step + 1, kind] = whole.astype(level_send.dtype)
                    level_copy(step + 1, kind).start()
            if not last:
                send_edges(step + 1, kind, 0)
        for kind in range(kinds):
            for turn in turns_of(1):
                inside(step, kind, turn, view(kind, turn))
            if parts > 1:
                take_edges(step, kind, 1, view)
                if not last:
                    send_edges(step + 1, kind, 1)

    barrier = pltpu.get_barrier_semaphore()
    for axis, here, size in (("row", me, count), ("mem", mem_at, mems), ("lev", lev_at, levs)):

        @pl.loop(1, size)
        def _(shift):
            pl.semaphore_signal(
                barrier, inc=1, device_id={axis: (here + shift) % size}, device_id_type=MESH
            )

    fetches = [
        pltpu.make_async_copy(taper.at[:, own_columns(mem_at)], taper_all.at[me], own_sem.at[0]),
        pltpu.make_async_copy(control, own, own_sem.at[1]),
        pltpu.make_async_copy(row_part, row_all.at[me], own_sem.at[2]),
        pltpu.make_async_copy(
            pert.at[:, :, :, :, own_columns(mem_at)], pert_all.at[mem_at], own_sem.at[3]
        ),
    ]
    late = [
        pltpu.make_async_copy(courant_in, courant, own_sem.at[4 + levels]),
        pltpu.make_async_copy(slope_in, slope, own_sem.at[5 + levels]),
    ]
    for level in range(levels):
        fetches.append(
            pltpu.make_async_copy(
                block(control, me, level), gathered.at[me, level], own_sem.at[4 + level]
            )
        )
    for fetch in fetches + late:
        fetch.start()
    for fetch in fetches[:3]:
        fetch.wait()
    pl.semaphore_wait(barrier, count + mems + levs - 3)

    if inner > 1:
        send(True, lambda: first(me, inner - 1 - side_at))
    along_line(0, 0)
    if inner > 1:
        send(True, lambda: side(me, side_at))
    for by in offsets:
        send(True, lambda by=by: row(peer_of(by), me))
    one_chunk(0)
    for shift in range(1, mems):
        send(True, lambda shift=shift: pert_copy((mem_at + shift) % mems, mem_at))
    for fetch in fetches[3:] + late:
        fetch.wait()
    set_factors()
    if inner > 1:
        first(other, side_at).wait_recv()
        along_line(0, 1)
        across(True, other, side_at)
    for turn in range(1, levels - 1):
        one_chunk(turn)
    if inner > 1:
        side(other, inner - 1 - side_at).wait_recv()
        across(True, other, inner - 1 - side_at)

    def hop_step(hop):
        for turn in range(inner):
            for way in range(2):
                origin, there, copy = line(way, hop, turn, False)

                def arrived(copy=copy):
                    copy().wait_recv()

                when(there, arrived)
                if hop + 1 < outer - 1:
                    _, onwards, relay = line(way, hop + 1, turn, True)
                    send(onwards, relay)
                if inner > 1:
                    send(there, lambda origin=origin: side(origin, side_at))
                across(there, origin, side_at)

    def side_step(hop):
        for turn in range(inner):
            for way in range(2):
                origin, there, _ = line(way, hop, turn, False)
                if inner > 1:

                    def arrived(origin=origin):
                        side(origin, inner - 1 - side_at).wait_recv()

                    when(there, arrived)
                    across(there, origin, inner - 1 - side_at)

    ready = 0
    for hop in range(outer - 1):
        hop_step(hop)
        if hop == 0:
            one_chunk(levels - 1)
            for by in offsets:
                slot = peer_of(by)
                row(slot, slot).wait_recv()
        if ready < levels:
            row_step(ready)
            ready += 1
        side_step(hop)
    for turn in range(ready, levels):
        row_step(turn)

    for turn in range(levels):
        level = level_of(turn)
        for by in offsets:
            slot = peer_of(by)
            two(slot, slot, level).wait_recv()
            for shift in range(1, mems):
                send(
                    True,
                    lambda shift=shift, slot=slot, level=level: onward(
                        (mem_at + shift) % mems, slot, level, mem_at
                    ),
                )

    for by in offsets:
        origin = peer_of(by)
        for at in range(inner):
            for shift in range(1, levs):
                lev_copy(origin, at, shift, False).wait_recv()
    for shift in range(1, mems):
        peer = (mem_at + shift) % mems
        pert_copy(peer, peer).wait_recv()

    span = min(width, 256)
    for turn in range(levels):
        level = level_of(turn)
        for shift in range(1, mems):
            peer = (mem_at + shift) % mems

            @pl.loop(0, count)
            def _(slot):
                onward(peer, slot, level, peer).wait_recv()

        for start in range(0, width, span):
            total = jnp.zeros((mems * members * rows, span), jnp.float32)
            for slot in range(count):
                total = total + jnp.dot(
                    halves[level, slot].reshape(mems * members * rows, depth),
                    taper_all[slot, :, pl.ds(start, span)],
                    preferred_element_type=jnp.float32,
                )
            for kind in range(kinds):
                weighted = jnp.zeros((rows, span), jnp.float32)
                for mem in range(mems):
                    for member in range(members):
                        at = (mem * members + member) * rows
                        weighted = weighted + pert_all[
                            mem, kind, member, level, :, pl.ds(start, span)
                        ].astype(jnp.float32) * total[at : at + rows]
                state[0, kind, turn, :, pl.ds(start, span)] = weighted
                if turn == 0 and levs > 1:
                    level_send[0, kind, :, pl.ds(start, span)] = weighted.astype(level_send.dtype)
        if turn == 0:
            for kind in range(kinds):
                if levs > 1:
                    level_copy(0, kind).start()
                send_edges(0, kind, 0)
    if parts > 1:
        for kind in range(kinds):
            send_edges(0, kind, 1)

    @pl.loop(0, STEPS - 1)
    def _(step):
        one_step(step, lambda kind, turn: state.at[step + 1, kind, turn], False)

    one_step(STEPS - 1, lambda kind, turn: out.at[kind, level_of(turn)], True)

    for there, copy in sent:
        when(there, lambda copy=copy: copy().wait_send())

    @pl.loop(0, STEPS)
    def _(step):
        for kind in range(kinds):
            if levs > 1:
                level_copy(step, kind).wait_send()
            for part in range(parts):
                for axis, at, there, target in neighbours:

                    @pl.when(there)
                    def _():
                        edge_copy(step, kind, part, axis, at, target, False).wait_send()


def on_device(
    control_fields, perturbations, column_taper, row_taper, courant_numbers, tracer_slope
):
    members, levels, rows, columns = control_fields.shape
    kinds = perturbations.shape[0]
    count, mems, levs = (lax.axis_size(axis) for axis in ("row", "mem", "lev"))
    depth, width = columns // count, columns // mems
    if depth % 128:
        control_fields = control_fields.reshape(members, levels, rows, count, depth)
        control_fields = control_fields.transpose(3, 0, 1, 2, 4)
    low, full, dma = jnp.bfloat16, jnp.float32, pltpu.SemaphoreType.DMA
    pairs = [dma((count, levels))] * 2 + [dma((count,))] * 2 + [dma((count, levels))] * 2
    pairs += [dma((mems, count, levels))] * 2 + [dma((mems,))] * 2 + [dma((1,))] * 2
    pairs += [dma((2, count, 2))] * 2 + [dma((count,))] * 2 + [dma((count, 2, levs))] * 2
    pairs += [dma((STEPS, kinds))] * 2 + [dma((STEPS, 2, kinds, 2))] * 4
    return pl.pallas_call(
        kernel,
        out_shape=jax.ShapeDtypeStruct((kinds, levels, rows, width), full),
        in_specs=[pl.BlockSpec(memory_space=pltpu.HBM)] * 6,
        out_specs=pl.BlockSpec(memory_space=pltpu.VMEM),
        scratch_shapes=[
            pltpu.VMEM(control_fields.shape, low),
            pltpu.VMEM((count, levels, members, rows, depth), low),
            pltpu.VMEM((count, rows, count * rows), low),
            pltpu.VMEM((count, levels, members, rows, depth), low),
            pltpu.VMEM((levels, count, mems, members, rows, depth), low),
            pltpu.VMEM((count, depth, width), low),
            pltpu.VMEM((mems, kinds, members, levels, rows, width), low),
            pltpu.VMEM(courant_numbers.shape, full),
            pltpu.VMEM(tracer_slope.shape, full),
            pltpu.VMEM((STEPS, kinds, levels, rows, width), full),
            pltpu.VMEM((7, levels, rows, width), full),
            pltpu.VMEM((STEPS, kinds, rows, width), low),
            pltpu.VMEM((STEPS, kinds, rows, width), low),
            pltpu.VMEM((STEPS, 2, kinds, levels, 1, width), full),
            pltpu.VMEM((STEPS, 2, kinds, levels, 1, width), full),
            pltpu.VMEM((STEPS, 2, kinds, levels, rows, 128), full),
            *pairs,
            dma((6 + levels,)),
        ],
        compiler_params=pltpu.CompilerParams(
            collective_id=0, has_side_effects=True, vmem_limit_bytes=44 << 20
        ),
        name="increment",
    )(
        *(
            pltpu.with_memory_space_constraint(operand, pltpu.HBM)
            for operand in (
                control_fields, perturbations, column_taper, row_taper, courant_numbers, tracer_slope
            )
        )
    )


def solution(mesh):
    assert mesh.shape["lev"] <= 2
    placed = (
        P("mem", "lev", "row", None),
        P(None, "mem", "lev", "row", None),
        P("row", None),
        P("row", None),
        P(None, "lev", "row", "mem"),
        P(None, "lev", "row", "mem"),
    )
    return jax.shard_map(
        on_device,
        mesh=mesh,
        in_specs=placed,
        out_specs=P(None, "lev", "row", "mem"),
        check_vma=False,
    )
```

```python
import jax
import jax.numpy as jnp
from jax import lax
from jax.experimental import pallas as pl
from jax.experimental.pallas import tpu as pltpu
from jax.sharding import PartitionSpec as P

STEPS = 4


MESH = pl.DeviceIdType.MESH


def kernel(
    control, pert, taper, row_part, courant_in, slope_in, out, own, gathered, row_all, staged, halves,
    taper_all, pert_all, courant, slope, state, factors, level_send, level_halo, row_edge, row_halo,
    column_halo, one_send, one_recv, row_send, row_recv, two_send, two_recv, pass_send, pass_recv,
    pert_send, pert_recv, first_send, first_recv, line_send, line_recv, side_send, side_recv, lev_send,
    lev_recv, up_send, up_recv, edge_send, edge_recv, column_send, column_recv, own_sem,
):
    count, mems, levs = (lax.axis_size(axis) for axis in ("row", "mem", "lev"))
    me, mem_at, lev_at = (lax.axis_index(axis) for axis in ("row", "mem", "lev"))
    kinds, members, levels, rows, columns = pert.shape
    depth, width = taper.shape[0], out.shape[3]
    inner = 2 if count % 2 == 0 else 1
    outer = count // inner
    line_at, side_at = me // inner, me % inner
    share, lanes = depth // levs, width // inner
    early = []

    def remote(source, landing, to, at, **target):
        return pltpu.make_async_remote_copy(
            src_ref=source, dst_ref=landing, send_sem=to, recv_sem=at, device_id=target,
            device_id_type=MESH,
        )

    def start(there, copy):
        when(there, lambda: copy().start())

    def send(there, copy):
        early.append((there, copy))
        start(there, copy)

    def when(there, action):
        if there is True:
            action()
        else:
            pl.when(there)(action)

    def own_columns(at):
        return pl.ds(pl.multiple_of(at * width, width), width)

    def block(source, at, level):
        if len(source.shape) == 5:
            return source.at[at, :, level]
        return source.at[:, level, :, pl.ds(pl.multiple_of(at * depth, depth), depth)]

    def level_of(turn):
        return jnp.where(lev_at > 0, turn, levels - 1 - turn)

    offsets = sorted(range(1, count), key=lambda by: -min(by // inner, outer - by // inner))

    def peer_of(by):
        return (line_at + by // inner) % outer * inner + (side_at + by % inner) % inner

    def one(peer, slot, level):
        return remote(
            block(own, peer, level), gathered.at[slot, level], one_send.at[0],
            one_recv.at[level], row=peer,
        )

    def row(peer, slot):
        return remote(row_all.at[me], row_all.at[slot], row_send.at[0], row_recv.at[0], row=peer)

    def two(peer, slot, level):
        return remote(
            staged.at[peer, level], halves.at[level, slot, mem_at], two_send.at[0],
            two_recv.at[level], row=peer,
        )

    def onward(peer, level, place):
        part = halves.at[level, :, place]
        return remote(part, part, pass_send.at[peer, level], pass_recv.at[place, level], mem=peer)

    def all_one(level):
        part = gathered.at[pl.ds(0, count - 1), level]
        return remote(part, part, one_send.at[0], one_recv.at[level], row=peer_of(1))

    def all_row():
        part = row_all.at[pl.ds(0, count - 1)]
        return remote(part, part, row_send.at[0], row_recv.at[0], row=peer_of(1))

    def all_two(level):
        part = gathered.at[pl.ds(0, count - 1), level]
        return remote(part, part, two_send.at[0], two_recv.at[level], row=peer_of(1))

    def all_sent(to):
        part = gathered.at[pl.ds(0, count - 1)]
        return remote(part, part, to, two_recv.at[0], row=peer_of(1))

    def all_side():
        part = taper_all.at[pl.ds(0, count - 1), pl.ds(0, share), pl.ds(0, lanes)]
        return remote(part, part, side_send.at[0], side_recv.at[0], row=peer_of(1))

    def all_lev():
        part = taper_all.at[pl.ds(0, count - 1), pl.ds(0, share)]
        return remote(part, part, lev_send.at[0], lev_recv.at[0], lev=levs - 1 - lev_at)

    def pert_copy(peer, slot):
        return remote(
            pert.at[:, :, :, :, own_columns(peer)], pert_all.at[slot], pert_send.at[peer],
            pert_recv.at[slot], mem=peer,
        )

    def piece(origin, lev, side):
        return taper_all.at[
            origin,
            pl.ds(pl.multiple_of(lev * share, share), share),
            pl.ds(pl.multiple_of(side * lanes, lanes), lanes),
        ]

    other = line_at * inner + (inner - 1 - side_at)

    def first(origin, side):
        part = piece(origin, lev_at, side)
        return remote(part, part, first_send.at[0], first_recv.at[0], row=other)

    def side(origin, at):
        part = piece(origin, lev_at, at)
        return remote(part, part, side_send.at[0], side_recv.at[origin], row=other)

    def line(way, hop, turn, sending):
        back = hop if sending else hop + 1
        from_line = line_at - back if way == 0 else line_at + back
        to_line = line_at + 1 if way == 0 else line_at - 1
        origin = from_line * inner + (side_at if turn == 0 else inner - 1 - side_at)
        there = from_line >= 0 if way == 0 else from_line <= outer - 1
        if sending:
            there = there & (to_line <= outer - 1 if way == 0 else to_line >= 0)

        def copy():
            part = piece(origin, lev_at, side_at)
            return remote(
                part, part, line_send.at[way, hop, turn], line_recv.at[way, hop, turn],
                row=to_line * inner + side_at,
            )

        return origin, there, copy

    def across(there, origin, at):
        def copy():
            part = piece(origin, lev_at, at)
            return remote(part, part, lev_send.at[0], lev_recv.at[0], lev=levs - 1 - lev_at)

        if levs > 1:
            start(there, copy)

    def along_line(hop, turn):
        if outer == 1:
            return
        for way in range(2):
            _, there, copy = line(way, hop, turn, True)
            send(there, copy)

    def one_chunk(turn, half=None):
        level = level_of(turn)
        cut = (len(offsets) + 1) // 2
        part = offsets if half is None else offsets[:cut] if half == 0 else offsets[cut:]
        for by in part:
            start(True, lambda by=by: one(peer_of(by), me, level))

    def row_step(turn):
        level = level_of(turn)
        if count > 1:
            all_one(level).wait_recv()
        whole = row_all[...].reshape(count * rows, count * rows)
        for member in range(members):
            tapered = jnp.dot(
                whole, gathered[:, level, member].reshape(count * rows, depth),
                preferred_element_type=jnp.float32,
            )
            staged[:, level, member] = tapered.astype(jnp.bfloat16).reshape(count, rows, depth)
        for by in offsets:
            start(True, lambda by=by: two(peer_of(by), me, level))
        for member in range(members):
            halves[level, me, mem_at, member] = staged[me, level, member]

    def set_factors():
        row_at = lax.broadcasted_iota(jnp.int32, (rows, width), 0)
        column_at = lax.broadcasted_iota(jnp.int32, (rows, width), 1)
        for turn in range(levels):
            level = level_of(turn)
            centre = jnp.ones((rows, width), jnp.float32)
            for at in range(3):
                speed = courant[at, level]
                ahead, back = jnp.maximum(speed, 0.0), -jnp.minimum(speed, 0.0)
                centre = centre - ahead - back
                if at == 0:
                    ahead, back = jnp.where(lev_at > 0, ahead, back), jnp.where(lev_at > 0, back, ahead)
                if at == 1:
                    ahead = jnp.where(row_at == 0, 0.0, ahead)
                    back = jnp.where(row_at == rows - 1, 0.0, back)
                if at == 2:
                    ahead = jnp.where(column_at == 0, 0.0, ahead)
                    back = jnp.where(column_at == width - 1, 0.0, back)
                factors[1 + 2 * at, turn] = ahead
                factors[2 + 2 * at, turn] = back
            factors[0, turn] = centre

    neighbours = []
    if count > 1:
        neighbours += [("row", 0, me > 0, me - 1), ("row", 1, me < count - 1, me + 1)]
    if mems > 1:
        neighbours += [("mem", 0, mem_at > 0, mem_at - 1), ("mem", 1, mem_at < mems - 1, mem_at + 1)]

    def part_of(turn):
        return min(turn, 1)

    def turns_of(part):
        return range(0, 1) if part == 0 else range(1, levels)

    parts = 1 if levels == 1 else 2

    def edge_copy(step, kind, part, axis, at, target, arriving):
        at_kind, turns = (kind, pl.ds(0, 1)) if part == 0 else (pl.ds(0, kinds), pl.ds(1, levels - 1))
        landed, slot = at if arriving else 1 - at, kind if part == 0 else kinds
        if axis == "row":
            source = row_edge.at[step, at, at_kind, turns]
            landing = row_halo.at[step, landed, at_kind, turns]
            to, there = edge_send.at[step, at], edge_recv.at[step % 2, landed, slot]
        else:
            source = state.at[step, at_kind, turns, :, pl.ds(0 if at == 0 else width - 128, 128)]
            landing = column_halo.at[step, landed, at_kind, turns]
            place = column_recv.shape[1]
            to, there = column_send.at[step, at % place], column_recv.at[step % 2, landed % place, slot]
        return remote(landing if arriving else source, landing, to, there, **{axis: target})

    def level_copy(step, kind):
        return remote(
            level_send.at[step, kind], level_halo.at[step, kind], up_send.at[step],
            up_recv.at[step % 2, kind], lev=levs - 1 - lev_at,
        )

    def send_edges(step, kind, part):
        for axis, at, there, target in neighbours:

            @pl.when(there)
            def _():
                if axis == "row":
                    for variable in [kind] if part == 0 else range(kinds):
                        for turn in turns_of(part):
                            row_edge[step, at, variable, turn] = state[
                                step, variable, turn, pl.ds(0 if at == 0 else rows - 1, 1)
                            ]
                edge_copy(step, kind, part, axis, at, target, False).start()

    def settle_step(step):
        if levs > 1:
            remote(
                level_send.at[step], level_send.at[step], up_send.at[step], up_recv.at[step % 2, 0],
                lev=levs - 1 - lev_at,
            ).wait_send()
        for axis, at, there, target in neighbours:

            @pl.when(there)
            def _():
                part = (row_edge if axis == "row" else column_halo).at[step, at]
                place = at % column_recv.shape[1]
                to = edge_send.at[step, at] if axis == "row" else column_send.at[step, place]
                remote(part, part, to, edge_recv.at[0, 0, 0], **{axis: target}).wait_send()

    def inside(step, kind, turn, target):
        here = state[step, kind, turn]
        new = here * factors[0, turn]
        new = new + factors[3, turn] * pltpu.roll(here, 1, 0)
        new = new + factors[4, turn] * pltpu.roll(here, rows - 1, 0)
        new = new + factors[5, turn] * pltpu.roll(here, 1, 1)
        new = new + factors[6, turn] * pltpu.roll(here, width - 1, 1)
        if turn > 0:
            new = new + factors[1, turn] * state[step, kind, turn - 1]
        if turn < levels - 1:
            new = new + factors[2, turn] * state[step, kind, turn + 1]
        if kind == 2:
            level = level_of(turn)
            new = new - (
                state[step, 0, turn] * slope[0, level] + state[step, 1, turn] * slope[1, level]
            )
        target[...] = new

    def take_edges(step, kind, part, view):
        lane_at = lax.broadcasted_iota(jnp.int32, (rows, 128), 1)
        for axis, at, there, target in neighbours:

            @pl.when(there)
            def _():
                edge_copy(step, kind, part, axis, at, target, True).wait_recv()
                whole = [kind] if part == 0 else range(kinds)
                for kind_at, turn in [(k, t) for k in whole for t in turns_of(part)]:
                    level, new = level_of(turn), view(kind_at, turn)
                    if axis == "row":
                        edge = pl.ds(0 if at == 0 else rows - 1, 1)
                        speed = courant[1, level, edge]
                        speed = -jnp.minimum(speed, 0.0) if at else jnp.maximum(speed, 0.0)
                        new[edge] = new[edge] + speed * row_halo[step, at, kind_at, turn]
                    else:
                        columns_at = pl.ds(width - 128 if at else 0, 128)
                        speed = courant[2, level, :, columns_at]
                        speed = -jnp.minimum(speed, 0.0) if at else jnp.maximum(speed, 0.0)
                        beside = pltpu.roll(
                            column_halo[step, at, kind_at, turn], 127 if at else 1, 1
                        )
                        new[:, columns_at] = new[:, columns_at] + jnp.where(
                            lane_at == (127 if at else 0), speed * beside, 0.0
                        )

    def one_step(step, view, last):
        for kind in range(kinds):
            inside(step, kind, 0, view(kind, 0))
        for kind in range(kinds):
            for turn in turns_of(1):
                inside(step, kind, turn, view(kind, turn))
            take_edges(step, kind, 0, view)
            if levs > 1:
                level_copy(step, kind).wait_recv()
                new = view(kind, 0)
                whole = new[...] + factors[1, 0] * level_halo[step, kind].astype(jnp.float32)
                new[...] = whole
                if not last:
                    level_send[step + 1, kind] = whole.astype(level_send.dtype)
                    level_copy(step + 1, kind).start()
            if not last:
                send_edges(step + 1, kind, 0)
        if parts > 1:
            take_edges(step, 0, 1, view)
            if not last:
                send_edges(step + 1, 0, 1)
        settle_step(step)

    barrier = pltpu.get_barrier_semaphore()
    for axis, here, size in (("row", me, count), ("mem", mem_at, mems), ("lev", lev_at, levs)):

        @pl.loop(1, size)
        def _(shift):
            pl.semaphore_signal(
                barrier, inc=1, device_id={axis: (here + shift) % size}, device_id_type=MESH
            )

    fetches = [
        pltpu.make_async_copy(taper.at[:, own_columns(mem_at)], taper_all.at[me], own_sem.at[0]),
        pltpu.make_async_copy(control, own, own_sem.at[1]),
        pltpu.make_async_copy(row_part, row_all.at[me], own_sem.at[2]),
        pltpu.make_async_copy(
            pert.at[:, :, :, :, own_columns(mem_at)], pert_all.at[mem_at], own_sem.at[3]
        ),
    ]
    late = [
        pltpu.make_async_copy(courant_in, courant, own_sem.at[4 + levels]),
        pltpu.make_async_copy(slope_in, slope, own_sem.at[5 + levels]),
    ]
    for level in range(levels):
        fetches.append(
            pltpu.make_async_copy(
                block(control, me, level), gathered.at[me, level], own_sem.at[4 + level]
            )
        )
    for fetch in fetches + late:
        fetch.start()
    for fetch in fetches[:3]:
        fetch.wait()
    pl.semaphore_wait(barrier, count + mems + levs - 3)

    if inner > 1:
        send(True, lambda: first(me, inner - 1 - side_at))
    along_line(0, 0)
    if inner > 1:
        start(True, lambda: side(me, side_at))
    for by in offsets:
        start(True, lambda by=by: row(peer_of(by), me))
    one_chunk(0)
    for shift in range(1, mems):
        send(True, lambda shift=shift: pert_copy((mem_at + shift) % mems, mem_at))
    for fetch in fetches[3:] + late:
        fetch.wait()
    set_factors()

    def hop_step(hop, turn):
        for way in range(2):
            origin, there, copy = line(way, hop, turn, False)

            def arrived(copy=copy):
                copy().wait_recv()

            when(there, arrived)
            if hop + 1 < outer - 1:
                _, onwards, relay = line(way, hop + 1, turn, True)
                send(onwards, relay)
            if inner > 1:
                start(there, lambda origin=origin: side(origin, side_at))
            across(there, origin, side_at)

    def side_step(hop):
        for turn in range(inner):
            for way in range(2):
                origin, there, _ = line(way, hop, turn, False)
                if inner > 1:

                    def arrived(origin=origin):
                        side(origin, inner - 1 - side_at).wait_recv()

                    when(there, arrived)
                    across(there, origin, inner - 1 - side_at)

    span = min(width, 256)

    def product_step(turn):
        level = level_of(turn)
        for shift in range(1, mems):
            peer = (mem_at + shift) % mems

            onward(peer, level, peer).wait_recv()

        for start in range(0, width, span):
            total = jnp.zeros((mems * members * rows, span), jnp.float32)
            for slot in range(count):
                total = total + jnp.dot(
                    halves[level, slot].reshape(mems * members * rows, depth),
                    taper_all[slot, :, pl.ds(start, span)],
                    preferred_element_type=jnp.float32,
                )
            for kind in range(kinds):
                weighted = jnp.zeros((rows, span), jnp.float32)
                for mem in range(mems):
                    for member in range(members):
                        at = (mem * members + member) * rows
                        weighted = weighted + pert_all[
                            mem, kind, member, level, :, pl.ds(start, span)
                        ].astype(jnp.float32) * total[at : at + rows]
                state[0, kind, turn, :, pl.ds(start, span)] = weighted
                if turn == 0 and levs > 1:
                    level_send[0, kind, :, pl.ds(start, span)] = weighted.astype(level_send.dtype)
        if turn == 0:
            for kind in range(kinds):
                if levs > 1:
                    level_copy(0, kind).start()
                send_edges(0, kind, 0)

    def first_step():
        if inner > 1:
            first(other, side_at).wait_recv()
            along_line(0, 1)
            across(True, other, side_at)

    def other_step():
        if inner > 1:
            side(other, inner - 1 - side_at).wait_recv()
            across(True, other, inner - 1 - side_at)

    def whole_row():
        if count > 1:
            all_row().wait_recv()

    def back_step(turn):
        level = level_of(turn)
        if count > 1:
            all_two(level).wait_recv()
        for shift in range(1, mems):
            onward((mem_at + shift) % mems, level, mem_at).start()

    def taper_whole():
        for there, copy in early:
            when(there, lambda copy=copy: copy().wait_send())
        if count > 1:
            all_row().wait_send()
            all_sent(one_send.at[0]).wait_send()
            if inner > 1:
                all_side().wait_send()
            if levs > 1:
                all_lev().wait_recv()
        for shift in range(1, mems):
            peer = (mem_at + shift) % mems
            pert_copy(peer, peer).wait_recv()

    def settle():
        if count > 1:
            all_sent(two_send.at[0]).wait_send()
            if levs > 1:
                all_lev().wait_send()
        for level in range(levels):
            for shift in range(1, mems):
                onward((mem_at + shift) % mems, level, mem_at).wait_send()

    first_step()
    chunks = [(turn, half) for turn in range(1, levels) for half in range(2)]
    turns_left, rows_known = list(range(levels)), False
    for hop in range(outer - 1):
        for turn in range(inner):
            hop_step(hop, turn)
            if chunks:
                one_chunk(*chunks.pop(0))
            if hop == 0 and turn == 0:
                other_step()
        if hop > 0 and not chunks and turns_left:
            if not rows_known:
                whole_row()
                rows_known = True
            row_step(turns_left.pop(0))
        side_step(hop)
        if 0 < hop < outer - 2 and rows_known and turns_left:
            row_step(turns_left.pop(0))
    if outer == 1:
        other_step()
    for turn, half in chunks:
        one_chunk(turn, half)
    if not rows_known:
        whole_row()
    for turn in turns_left:
        row_step(turn)
    for turn in range(levels - 1):
        back_step(turn)
    taper_whole()
    for turn in range(levels - 1):
        product_step(turn)
    back_step(levels - 1)
    product_step(levels - 1)
    if parts > 1:
        send_edges(0, 0, 1)
    settle()

    @pl.loop(0, STEPS - 1)
    def _(step):
        one_step(step, lambda kind, turn: state.at[step + 1, kind, turn], False)

    one_step(STEPS - 1, lambda kind, turn: out.at[kind, level_of(turn)], True)


def on_device(
    control_fields, perturbations, column_taper, row_taper, courant_numbers, tracer_slope
):
    members, levels, rows, columns = control_fields.shape
    kinds = perturbations.shape[0]
    count, mems, levs = (lax.axis_size(axis) for axis in ("row", "mem", "lev"))
    depth, width = columns // count, columns // mems
    if depth % 128:
        control_fields = control_fields.reshape(members, levels, rows, count, depth)
        control_fields = control_fields.transpose(3, 0, 1, 2, 4)
    low, full, dma = jnp.bfloat16, jnp.float32, pltpu.SemaphoreType.DMA
    inner = 2 if count % 2 == 0 else 1
    sides, hops = max(1, min(2, mems - 1)), max(1, count // inner - 1)
    semaphores = [dma((1,)), dma((levels,)), dma((1,)), dma((1,)), dma((1,)), dma((levels,))]
    semaphores += [dma((mems, levels))] * 2 + [dma((mems,))] * 2 + [dma((1,))] * 2
    semaphores += [dma((2, hops, inner))] * 2 + [dma((1,)), dma((count,)), dma((1,)), dma((1,))]
    semaphores += [dma((STEPS,)), dma((2, kinds)), dma((STEPS, 2)), dma((2, 2, kinds + 1))]
    semaphores += [dma((STEPS, sides)), dma((2, sides, kinds + 1))]
    return pl.pallas_call(
        kernel,
        out_shape=jax.ShapeDtypeStruct((kinds, levels, rows, width), full),
        in_specs=[pl.BlockSpec(memory_space=pltpu.HBM)] * 6,
        out_specs=pl.BlockSpec(memory_space=pltpu.VMEM),
        scratch_shapes=[
            pltpu.VMEM(control_fields.shape, low),
            pltpu.VMEM((count, levels, members, rows, depth), low),
            pltpu.VMEM((count, rows, count * rows), low),
            pltpu.VMEM((count, levels, members, rows, depth), low),
            pltpu.VMEM((levels, count, mems, members, rows, depth), low),
            pltpu.VMEM((count, depth, width), low),
            pltpu.VMEM((mems, kinds, members, levels, rows, width), low),
            pltpu.VMEM(courant_numbers.shape, full),
            pltpu.VMEM(tracer_slope.shape, full),
            pltpu.VMEM((STEPS, kinds, levels, rows, width), full),
            pltpu.VMEM((7, levels, rows, width), full),
            pltpu.VMEM((STEPS, kinds, rows, width), low),
            pltpu.VMEM((STEPS, kinds, rows, width), low),
            pltpu.VMEM((STEPS, 2, kinds, levels, 1, width), full),
            pltpu.VMEM((STEPS, 2, kinds, levels, 1, width), full),
            pltpu.VMEM((STEPS, 2, kinds, levels, rows, 128), full),
            *semaphores,
            dma((6 + levels,)),
        ],
        compiler_params=pltpu.CompilerParams(
            collective_id=0, has_side_effects=True, vmem_limit_bytes=44 << 20
        ),
        name="increment",
    )(
        *(
            pltpu.with_memory_space_constraint(operand, pltpu.HBM)
            for operand in (
                control_fields, perturbations, column_taper, row_taper, courant_numbers, tracer_slope
            )
        )
    )


def solution(mesh):
    assert mesh.shape["lev"] <= 2
    placed = (
        P("mem", "lev", "row", None),
        P(None, "mem", "lev", "row", None),
        P("row", None),
        P("row", None),
        P(None, "lev", "row", "mem"),
        P(None, "lev", "row", "mem"),
    )
    return jax.shard_map(
        on_device,
        mesh=mesh,
        in_specs=placed,
        out_specs=P(None, "lev", "row", "mem"),
        check_vma=False,
    )
```

```python
import jax
import jax.numpy as jnp
from jax import lax
from jax.experimental import pallas as pl
from jax.experimental.pallas import tpu as pltpu
from jax.sharding import PartitionSpec as P

STEPS = 4


MESH = pl.DeviceIdType.MESH


def kernel(
    control, pert, taper, row_part, courant_in, slope_in, out, own, gathered, row_all, staged, halves,
    taper_all, pert_all, courant, slope, state, factors, level_send, level_halo, row_edge, row_halo,
    column_halo, one_send, one_recv, row_send, row_recv, two_send, two_recv, pass_send, pass_recv,
    pert_send, pert_recv, first_send, first_recv, line_send, line_recv, side_send, side_recv, lev_send,
    lev_recv, up_send, up_recv, edge_send, edge_recv, column_send, column_recv, own_sem,
):
    count, mems, levs = (lax.axis_size(axis) for axis in ("row", "mem", "lev"))
    me, mem_at, lev_at = (lax.axis_index(axis) for axis in ("row", "mem", "lev"))
    kinds, members, levels, rows, columns = pert.shape
    depth, width = taper.shape[0], out.shape[3]
    inner = 2 if count % 2 == 0 else 1
    outer = count // inner
    line_at, side_at = me // inner, me % inner
    share, lanes = depth // levs, width // inner
    early = []

    def remote(source, landing, to, at, **target):
        return pltpu.make_async_remote_copy(
            src_ref=source, dst_ref=landing, send_sem=to, recv_sem=at, device_id=target,
            device_id_type=MESH,
        )

    def start(there, copy):
        when(there, lambda: copy().start())

    def send(there, copy):
        early.append((there, copy))
        start(there, copy)

    def when(there, action):
        if there is True:
            action()
        else:
            pl.when(there)(action)

    def own_columns(at):
        return pl.ds(pl.multiple_of(at * width, width), width)

    def block(source, at, level):
        if len(source.shape) == 5:
            return source.at[at, :, level]
        return source.at[:, level, :, pl.ds(pl.multiple_of(at * depth, depth), depth)]

    def level_of(turn):
        return jnp.where(lev_at > 0, turn, levels - 1 - turn)

    offsets = sorted(range(1, count), key=lambda by: -min(by // inner, outer - by // inner))

    def peer_of(by):
        return (line_at + by // inner) % outer * inner + (side_at + by % inner) % inner

    def one(peer, slot, level):
        return remote(
            block(own, peer, level), gathered.at[slot, level], one_send.at[0],
            one_recv.at[level], row=peer,
        )

    def row(peer, slot):
        return remote(row_all.at[me], row_all.at[slot], row_send.at[0], row_recv.at[0], row=peer)

    def two(peer, slot, level):
        return remote(
            staged.at[peer, level], halves.at[level, slot, mem_at], two_send.at[0],
            two_recv.at[level], row=peer,
        )

    def onward(peer, level, place):
        part = halves.at[level, :, place]
        return remote(part, part, pass_send.at[peer, level], pass_recv.at[place, level], mem=peer)

    def all_one(level):
        part = gathered.at[pl.ds(0, count - 1), level]
        return remote(part, part, one_send.at[0], one_recv.at[level], row=peer_of(1))

    def all_row():
        part = row_all.at[pl.ds(0, count - 1)]
        return remote(part, part, row_send.at[0], row_recv.at[0], row=peer_of(1))

    def all_two(level):
        part = gathered.at[pl.ds(0, count - 1), level]
        return remote(part, part, two_send.at[0], two_recv.at[level], row=peer_of(1))

    def all_sent(to):
        part = gathered.at[pl.ds(0, count - 1)]
        return remote(part, part, to, two_recv.at[0], row=peer_of(1))

    def all_side():
        part = taper_all.at[pl.ds(0, count - 1), pl.ds(0, share), pl.ds(0, lanes)]
        return remote(part, part, side_send.at[0], side_recv.at[0], row=peer_of(1))

    def all_lev(blocks):
        part = taper_all.at[pl.ds(0, blocks), pl.ds(0, share)]
        return remote(part, part, lev_send.at[0], lev_recv.at[0], lev=levs - 1 - lev_at)

    corners = inner > 1 and levs > 1 and outer > 1
    at_end = (line_at == 0) | (line_at == outer - 1)
    far = jnp.where(line_at == 0, outer - 1, 0) * inner + inner - 1

    def corner(lev):
        part = piece(far, lev, side_at)
        return remote(part, part, lev_send.at[1], lev_recv.at[1], lev=levs - 1 - lev_at)

    def opposite(at):
        part = piece(far, levs - 1 - lev_at, at)
        return remote(part, part, first_send.at[1], first_recv.at[1], row=other)

    def each_lev(action):
        if corners:
            pl.when(at_end)(lambda: action(all_lev(count - 2)))
            pl.when(jnp.logical_not(at_end))(lambda: action(all_lev(count - 1)))
        else:
            action(all_lev(count - 1))

    def pert_copy(peer, slot):
        return remote(
            pert.at[:, :, :, :, own_columns(peer)], pert_all.at[slot], pert_send.at[peer],
            pert_recv.at[slot], mem=peer,
        )

    def piece(origin, lev, side):
        return taper_all.at[
            origin,
            pl.ds(pl.multiple_of(lev * share, share), share),
            pl.ds(pl.multiple_of(side * lanes, lanes), lanes),
        ]

    other = line_at * inner + (inner - 1 - side_at)

    def first(origin, side):
        part = piece(origin, lev_at, side)
        return remote(part, part, first_send.at[0], first_recv.at[0], row=other)

    def side(origin, at):
        part = piece(origin, lev_at, at)
        return remote(part, part, side_send.at[0], side_recv.at[origin], row=other)

    def line(way, hop, turn, sending):
        back = hop if sending else hop + 1
        from_line = line_at - back if way == 0 else line_at + back
        to_line = line_at + 1 if way == 0 else line_at - 1
        origin = from_line * inner + (side_at if turn == 0 else inner - 1 - side_at)
        there = from_line >= 0 if way == 0 else from_line <= outer - 1
        if sending:
            there = there & (to_line <= outer - 1 if way == 0 else to_line >= 0)

        def copy():
            part = piece(origin, lev_at, side_at)
            return remote(
                part, part, line_send.at[way, hop, turn], line_recv.at[way, hop, turn],
                row=to_line * inner + side_at,
            )

        return origin, there, copy

    def across(there, origin, at):
        def copy():
            part = piece(origin, lev_at, at)
            return remote(part, part, lev_send.at[0], lev_recv.at[0], lev=levs - 1 - lev_at)

        if levs > 1:
            start(there, copy)

    def along_line(hop, turn):
        if outer == 1:
            return
        for way in range(2):
            _, there, copy = line(way, hop, turn, True)
            send(there, copy)

    def one_chunk(turn, half=None):
        level = level_of(turn)
        cut = (len(offsets) + 1) // 2
        part = offsets if half is None else offsets[:cut] if half == 0 else offsets[cut:]
        for by in part:
            start(True, lambda by=by: one(peer_of(by), me, level))

    def row_step(turn):
        level = level_of(turn)
        if count > 1:
            all_one(level).wait_recv()
        whole = row_all[...].reshape(count * rows, count * rows)
        for member in range(members):
            tapered = jnp.dot(
                whole, gathered[:, level, member].reshape(count * rows, depth),
                preferred_element_type=jnp.float32,
            )
            staged[:, level, member] = tapered.astype(jnp.bfloat16).reshape(count, rows, depth)
        for by in offsets:
            start(True, lambda by=by: two(peer_of(by), me, level))
        for member in range(members):
            halves[level, me, mem_at, member] = staged[me, level, member]

    def set_factors():
        row_at = lax.broadcasted_iota(jnp.int32, (rows, width), 0)
        column_at = lax.broadcasted_iota(jnp.int32, (rows, width), 1)
        for turn in range(levels):
            level = level_of(turn)
            centre = jnp.ones((rows, width), jnp.float32)
            for at in range(3):
                speed = courant[at, level]
                ahead, back = jnp.maximum(speed, 0.0), -jnp.minimum(speed, 0.0)
                centre = centre - ahead - back
                if at == 0:
                    ahead, back = jnp.where(lev_at > 0, ahead, back), jnp.where(lev_at > 0, back, ahead)
                if at == 1:
                    ahead = jnp.where(row_at == 0, 0.0, ahead)
                    back = jnp.where(row_at == rows - 1, 0.0, back)
                if at == 2:
                    ahead = jnp.where(column_at == 0, 0.0, ahead)
                    back = jnp.where(column_at == width - 1, 0.0, back)
                factors[1 + 2 * at, turn] = ahead
                factors[2 + 2 * at, turn] = back
            factors[0, turn] = centre

    neighbours = []
    if count > 1:
        neighbours += [("row", 0, me > 0, me - 1), ("row", 1, me < count - 1, me + 1)]
    if mems > 1:
        neighbours += [("mem", 0, mem_at > 0, mem_at - 1), ("mem", 1, mem_at < mems - 1, mem_at + 1)]

    def part_of(turn):
        return min(turn, 1)

    def turns_of(part):
        return range(0, 1) if part == 0 else range(1, levels)

    parts = 1 if levels == 1 else 2

    def edge_copy(step, kind, part, axis, at, target, arriving):
        at_kind, turns = (kind, pl.ds(0, 1)) if part == 0 else (pl.ds(0, kinds), pl.ds(1, levels - 1))
        landed, slot = at if arriving else 1 - at, kind if part == 0 else kinds
        if axis == "row":
            source = row_edge.at[step, at, at_kind, turns]
            landing = row_halo.at[step, landed, at_kind, turns]
            to, there = edge_send.at[step, at], edge_recv.at[step % 2, landed, slot]
        else:
            source = state.at[step, at_kind, turns, :, pl.ds(0 if at == 0 else width - 128, 128)]
            landing = column_halo.at[step, landed, at_kind, turns]
            place = column_recv.shape[1]
            to, there = column_send.at[step, at % place], column_recv.at[step % 2, landed % place, slot]
        return remote(landing if arriving else source, landing, to, there, **{axis: target})

    def level_copy(step, kind):
        return remote(
            level_send.at[step, kind], level_halo.at[step, kind], up_send.at[step],
            up_recv.at[step % 2, kind], lev=levs - 1 - lev_at,
        )

    def send_edges(step, kind, part):
        for axis, at, there, target in neighbours:

            @pl.when(there)
            def _():
                if axis == "row":
                    for variable in [kind] if part == 0 else range(kinds):
                        for turn in turns_of(part):
                            row_edge[step, at, variable, turn] = state[
                                step, variable, turn, pl.ds(0 if at == 0 else rows - 1, 1)
                            ]
                edge_copy(step, kind, part, axis, at, target, False).start()

    def settle_step(step):
        if levs > 1:
            remote(
                level_send.at[step], level_send.at[step], up_send.at[step], up_recv.at[step % 2, 0],
                lev=levs - 1 - lev_at,
            ).wait_send()
        for axis, at, there, target in neighbours:

            @pl.when(there)
            def _():
                part = (row_edge if axis == "row" else column_halo).at[step, at]
                place = at % column_recv.shape[1]
                to = edge_send.at[step, at] if axis == "row" else column_send.at[step, place]
                remote(part, part, to, edge_recv.at[0, 0, 0], **{axis: target}).wait_send()

    def inside(step, kind, turn, target):
        here = state[step, kind, turn]
        new = here * factors[0, turn]
        new = new + factors[3, turn] * pltpu.roll(here, 1, 0)
        new = new + factors[4, turn] * pltpu.roll(here, rows - 1, 0)
        new = new + factors[5, turn] * pltpu.roll(here, 1, 1)
        new = new + factors[6, turn] * pltpu.roll(here, width - 1, 1)
        if turn > 0:
            new = new + factors[1, turn] * state[step, kind, turn - 1]
        if turn < levels - 1:
            new = new + factors[2, turn] * state[step, kind, turn + 1]
        if kind == 2:
            level = level_of(turn)
            new = new - (
                state[step, 0, turn] * slope[0, level] + state[step, 1, turn] * slope[1, level]
            )
        target[...] = new

    def take_edges(step, kind, part, view):
        lane_at = lax.broadcasted_iota(jnp.int32, (rows, 128), 1)
        for axis, at, there, target in neighbours:

            @pl.when(there)
            def _():
                edge_copy(step, kind, part, axis, at, target, True).wait_recv()
                whole = [kind] if part == 0 else range(kinds)
                for kind_at, turn in [(k, t) for k in whole for t in turns_of(part)]:
                    level, new = level_of(turn), view(kind_at, turn)
                    if axis == "row":
                        edge = pl.ds(0 if at == 0 else rows - 1, 1)
                        speed = courant[1, level, edge]
                        speed = -jnp.minimum(speed, 0.0) if at else jnp.maximum(speed, 0.0)
                        new[edge] = new[edge] + speed * row_halo[step, at, kind_at, turn]
                    else:
                        columns_at = pl.ds(width - 128 if at else 0, 128)
                        speed = courant[2, level, :, columns_at]
                        speed = -jnp.minimum(speed, 0.0) if at else jnp.maximum(speed, 0.0)
                        beside = pltpu.roll(
                            column_halo[step, at, kind_at, turn], 127 if at else 1, 1
                        )
                        new[:, columns_at] = new[:, columns_at] + jnp.where(
                            lane_at == (127 if at else 0), speed * beside, 0.0
                        )

    def one_step(step, view, last):
        for kind in range(kinds):
            inside(step, kind, 0, view(kind, 0))
        for kind in range(kinds):
            for turn in turns_of(1):
                inside(step, kind, turn, view(kind, turn))
            take_edges(step, kind, 0, view)
            if levs > 1:
                level_copy(step, kind).wait_recv()
                new = view(kind, 0)
                whole = new[...] + factors[1, 0] * level_halo[step, kind].astype(jnp.float32)
                new[...] = whole
                if not last:
                    level_send[step + 1, kind] = whole.astype(level_send.dtype)
                    level_copy(step + 1, kind).start()
            if not last:
                send_edges(step + 1, kind, 0)
        if parts > 1:
            take_edges(step, 0, 1, view)
            if not last:
                send_edges(step + 1, 0, 1)
        settle_step(step)

    barrier = pltpu.get_barrier_semaphore()
    for axis, here, size in (("row", me, count), ("mem", mem_at, mems), ("lev", lev_at, levs)):

        @pl.loop(1, size)
        def _(shift):
            pl.semaphore_signal(
                barrier, inc=1, device_id={axis: (here + shift) % size}, device_id_type=MESH
            )

    fetches = [
        pltpu.make_async_copy(taper.at[:, own_columns(mem_at)], taper_all.at[me], own_sem.at[0]),
        pltpu.make_async_copy(control, own, own_sem.at[1]),
        pltpu.make_async_copy(row_part, row_all.at[me], own_sem.at[2]),
        pltpu.make_async_copy(
            pert.at[:, :, :, :, own_columns(mem_at)], pert_all.at[mem_at], own_sem.at[3]
        ),
    ]
    late = [
        pltpu.make_async_copy(courant_in, courant, own_sem.at[4 + levels]),
        pltpu.make_async_copy(slope_in, slope, own_sem.at[5 + levels]),
    ]
    for level in range(levels):
        fetches.append(
            pltpu.make_async_copy(
                block(control, me, level), gathered.at[me, level], own_sem.at[4 + level]
            )
        )
    for fetch in fetches + late:
        fetch.start()
    for fetch in fetches[:3]:
        fetch.wait()
    pl.semaphore_wait(barrier, count + mems + levs - 3)

    if inner > 1:
        send(True, lambda: first(me, inner - 1 - side_at))
    along_line(0, 0)
    if inner > 1:
        start(True, lambda: side(me, side_at))
    for by in offsets:
        start(True, lambda by=by: row(peer_of(by), me))
    one_chunk(0)
    for shift in range(1, mems):
        send(True, lambda shift=shift: pert_copy((mem_at + shift) % mems, mem_at))
    for fetch in fetches[3:] + late:
        fetch.wait()
    set_factors()

    def hop_step(hop, turn):
        for way in range(2):
            origin, there, copy = line(way, hop, turn, False)

            def arrived(copy=copy):
                copy().wait_recv()

            when(there, arrived)
            if hop + 1 < outer - 1:
                _, onwards, relay = line(way, hop + 1, turn, True)
                send(onwards, relay)
            if inner > 1:
                start(there, lambda origin=origin: side(origin, side_at))
            if corners and hop == outer - 2:
                across(there & (side_at == turn), origin, side_at)
                start(there & (side_at != turn), lambda: corner(lev_at))
            else:
                across(there, origin, side_at)

    def side_step(hop):
        for turn in range(inner):
            for way in range(2):
                origin, there, _ = line(way, hop, turn, False)
                if inner > 1:

                    def arrived(origin=origin):
                        side(origin, inner - 1 - side_at).wait_recv()

                    when(there, arrived)
                    if corners and hop == outer - 2:
                        across(there & (side_at == turn), origin, inner - 1 - side_at)
                    else:
                        across(there, origin, inner - 1 - side_at)
        if corners and hop == outer - 2:

            @pl.when(at_end)
            def _():
                corner(levs - 1 - lev_at).wait_recv()
                opposite(side_at).start()

    span = min(width, 256)

    def product_step(turn):
        level = level_of(turn)
        for shift in range(1, mems):
            peer = (mem_at + shift) % mems

            onward(peer, level, peer).wait_recv()

        for start in range(0, width, span):
            total = jnp.zeros((mems * members * rows, span), jnp.float32)
            for slot in range(count):
                total = total + jnp.dot(
                    halves[level, slot].reshape(mems * members * rows, depth),
                    taper_all[slot, :, pl.ds(start, span)],
                    preferred_element_type=jnp.float32,
                )
            for kind in range(kinds):
                weighted = jnp.zeros((rows, span), jnp.float32)
                for mem in range(mems):
                    for member in range(members):
                        at = (mem * members + member) * rows
                        weighted = weighted + pert_all[
                            mem, kind, member, level, :, pl.ds(start, span)
                        ].astype(jnp.float32) * total[at : at + rows]
                state[0, kind, turn, :, pl.ds(start, span)] = weighted
                if turn == 0 and levs > 1:
                    level_send[0, kind, :, pl.ds(start, span)] = weighted.astype(level_send.dtype)
        if turn == 0:
            for kind in range(kinds):
                if levs > 1:
                    level_copy(0, kind).start()
                send_edges(0, kind, 0)

    def first_step():
        if inner > 1:
            first(other, side_at).wait_recv()
            along_line(0, 1)
            across(True, other, side_at)

    def other_step():
        if inner > 1:
            side(other, inner - 1 - side_at).wait_recv()
            across(True, other, inner - 1 - side_at)

    def whole_row():
        if count > 1:
            all_row().wait_recv()

    def back_step(turn):
        level = level_of(turn)
        if count > 1:
            all_two(level).wait_recv()
        for shift in range(1, mems):
            onward((mem_at + shift) % mems, level, mem_at).start()

    def taper_whole():
        for there, copy in early:
            when(there, lambda copy=copy: copy().wait_send())
        if count > 1:
            all_row().wait_send()
            all_sent(one_send.at[0]).wait_send()
            if inner > 1:
                all_side().wait_send()
            if levs > 1:
                each_lev(lambda copy: copy.wait_recv())
            if corners:

                @pl.when(at_end)
                def _():
                    opposite(inner - 1 - side_at).wait_recv()
        for shift in range(1, mems):
            peer = (mem_at + shift) % mems
            pert_copy(peer, peer).wait_recv()

    def settle():
        if count > 1:
            all_sent(two_send.at[0]).wait_send()
            if levs > 1:
                each_lev(lambda copy: copy.wait_send())
            if corners:

                @pl.when(at_end)
                def _():
                    corner(lev_at).wait_send()
                    opposite(side_at).wait_send()
        for level in range(levels):
            for shift in range(1, mems):
                onward((mem_at + shift) % mems, level, mem_at).wait_send()

    first_step()
    chunks = [(turn, half) for turn in range(1, levels) for half in range(2)]
    turns_left = list(range(levels))

    def next_chunk():
        if chunks:
            one_chunk(*chunks.pop(0))

    def next_row():
        if turns_left:
            turn = turns_left.pop(0)
            while chunks and chunks[0][0] <= turn:
                next_chunk()
            if turn == 0:
                whole_row()
            row_step(turn)

    for hop in range(outer - 1):
        hop_step(hop, 0)
        if hop == 0:
            next_chunk()
            other_step()
        if hop == 1:
            side_step(0)
        for turn in range(1, inner):
            hop_step(hop, turn)
        if hop == 0:
            next_chunk()
            if outer == 2:
                side_step(0)
        elif hop < outer - 2:
            next_chunk()
            side_step(hop)
            next_row()
            next_chunk()
            next_row()
        else:
            next_row()
            side_step(hop)
    if outer == 1:
        other_step()
    for _ in range(levels):
        next_row()
    for turn in range(levels - 1):
        back_step(turn)
    taper_whole()
    for turn in range(levels - 1):
        product_step(turn)
    back_step(levels - 1)
    product_step(levels - 1)
    if parts > 1:
        send_edges(0, 0, 1)
    settle()

    @pl.loop(0, STEPS - 1)
    def _(step):
        one_step(step, lambda kind, turn: state.at[step + 1, kind, turn], False)

    one_step(STEPS - 1, lambda kind, turn: out.at[kind, level_of(turn)], True)


def on_device(
    control_fields, perturbations, column_taper, row_taper, courant_numbers, tracer_slope
):
    members, levels, rows, columns = control_fields.shape
    kinds = perturbations.shape[0]
    count, mems, levs = (lax.axis_size(axis) for axis in ("row", "mem", "lev"))
    depth, width = columns // count, columns // mems
    if depth % 128:
        control_fields = control_fields.reshape(members, levels, rows, count, depth)
        control_fields = control_fields.transpose(3, 0, 1, 2, 4)
    low, full, dma = jnp.bfloat16, jnp.float32, pltpu.SemaphoreType.DMA
    inner = 2 if count % 2 == 0 else 1
    sides, hops = max(1, min(2, mems - 1)), max(1, count // inner - 1)
    semaphores = [dma((1,)), dma((levels,)), dma((1,)), dma((1,)), dma((1,)), dma((levels,))]
    semaphores += [dma((mems, levels))] * 2 + [dma((mems,))] * 2 + [dma((2,))] * 2
    semaphores += [dma((2, hops, inner))] * 2 + [dma((1,)), dma((count,)), dma((2,)), dma((2,))]
    semaphores += [dma((STEPS,)), dma((2, kinds)), dma((STEPS, 2)), dma((2, 2, kinds + 1))]
    semaphores += [dma((STEPS, sides)), dma((2, sides, kinds + 1))]
    return pl.pallas_call(
        kernel,
        out_shape=jax.ShapeDtypeStruct((kinds, levels, rows, width), full),
        in_specs=[pl.BlockSpec(memory_space=pltpu.HBM)] * 6,
        out_specs=pl.BlockSpec(memory_space=pltpu.VMEM),
        scratch_shapes=[
            pltpu.VMEM(control_fields.shape, low),
            pltpu.VMEM((count, levels, members, rows, depth), low),
            pltpu.VMEM((count, rows, count * rows), low),
            pltpu.VMEM((count, levels, members, rows, depth), low),
            pltpu.VMEM((levels, count, mems, members, rows, depth), low),
            pltpu.VMEM((count, depth, width), low),
            pltpu.VMEM((mems, kinds, members, levels, rows, width), low),
            pltpu.VMEM(courant_numbers.shape, full),
            pltpu.VMEM(tracer_slope.shape, full),
            pltpu.VMEM((STEPS, kinds, levels, rows, width), full),
            pltpu.VMEM((7, levels, rows, width), full),
            pltpu.VMEM((STEPS, kinds, rows, width), low),
            pltpu.VMEM((STEPS, kinds, rows, width), low),
            pltpu.VMEM((STEPS, 2, kinds, levels, 1, width), full),
            pltpu.VMEM((STEPS, 2, kinds, levels, 1, width), full),
            pltpu.VMEM((STEPS, 2, kinds, levels, rows, 128), full),
            *semaphores,
            dma((6 + levels,)),
        ],
        compiler_params=pltpu.CompilerParams(
            collective_id=0, has_side_effects=True, vmem_limit_bytes=44 << 20
        ),
        name="increment",
    )(
        *(
            pltpu.with_memory_space_constraint(operand, pltpu.HBM)
            for operand in (
                control_fields, perturbations, column_taper, row_taper, courant_numbers, tracer_slope
            )
        )
    )


def solution(mesh):
    assert mesh.shape["lev"] <= 2
    placed = (
        P("mem", "lev", "row", None),
        P(None, "mem", "lev", "row", None),
        P("row", None),
        P("row", None),
        P(None, "lev", "row", "mem"),
        P(None, "lev", "row", "mem"),
    )
    return jax.shard_map(
        on_device,
        mesh=mesh,
        in_specs=placed,
        out_specs=P(None, "lev", "row", "mem"),
        check_vma=False,
    )
```

```python
import jax
import jax.numpy as jnp
from jax import lax
from jax.experimental import pallas as pl
from jax.experimental.pallas import tpu as pltpu
from jax.sharding import PartitionSpec as P

STEPS = 4


MESH = pl.DeviceIdType.MESH


def kernel(
    control, pert, taper, row_part, courant_in, slope_in, out, own, gathered, row_all, staged, halves,
    taper_all, pert_all, courant, slope, state, factors, level_send, level_halo, row_edge, row_halo,
    column_halo, one_send, one_recv, row_send, row_recv, two_send, two_recv, pass_send, pass_recv,
    pert_send, pert_recv, first_send, first_recv, line_send, line_recv, side_send, side_recv, lev_send,
    lev_recv, up_send, up_recv, edge_send, edge_recv, column_send, column_recv, own_sem,
):
    count, mems, levs = (lax.axis_size(axis) for axis in ("row", "mem", "lev"))
    me, mem_at, lev_at = (lax.axis_index(axis) for axis in ("row", "mem", "lev"))
    kinds, members, levels, rows, columns = pert.shape
    depth, width = taper.shape[0], out.shape[3]
    inner = 2 if count % 2 == 0 else 1
    outer = count // inner
    line_at, side_at = me // inner, me % inner
    share, lanes = depth // levs, width // inner
    early = []

    def remote(source, landing, to, at, **target):
        return pltpu.make_async_remote_copy(
            src_ref=source, dst_ref=landing, send_sem=to, recv_sem=at, device_id=target,
            device_id_type=MESH,
        )

    def start(there, copy):
        when(there, lambda: copy().start())

    def send(there, copy):
        early.append((there, copy))
        start(there, copy)

    def when(there, action):
        if there is True:
            action()
        else:
            pl.when(there)(action)

    def own_columns(at):
        return pl.ds(pl.multiple_of(at * width, width), width)

    def block(source, at, level):
        if len(source.shape) == 5:
            return source.at[at, :, level]
        return source.at[:, level, :, pl.ds(pl.multiple_of(at * depth, depth), depth)]

    def level_of(turn):
        return jnp.where(lev_at > 0, turn, levels - 1 - turn)

    offsets = sorted(range(1, count), key=lambda by: -min(by // inner, outer - by // inner))

    def peer_of(by):
        return (line_at + by // inner) % outer * inner + (side_at + by % inner) % inner

    def one(peer, slot, level):
        return remote(
            block(own, peer, level), gathered.at[slot, level], one_send.at[0],
            one_recv.at[level], row=peer,
        )

    def row(peer, slot):
        return remote(row_all.at[me], row_all.at[slot], row_send.at[0], row_recv.at[0], row=peer)

    def two(peer, slot, level):
        return remote(
            staged.at[peer, level], halves.at[level, slot, mem_at], two_send.at[0],
            two_recv.at[level], row=peer,
        )

    def onward(peer, level, place):
        part = halves.at[level, :, place]
        return remote(part, part, pass_send.at[peer, level], pass_recv.at[place, level], mem=peer)

    def all_one(level):
        part = gathered.at[pl.ds(0, count - 1), level]
        return remote(part, part, one_send.at[0], one_recv.at[level], row=peer_of(1))

    def all_row():
        part = row_all.at[pl.ds(0, count - 1)]
        return remote(part, part, row_send.at[0], row_recv.at[0], row=peer_of(1))

    def all_two(level):
        part = gathered.at[pl.ds(0, count - 1), level]
        return remote(part, part, two_send.at[0], two_recv.at[level], row=peer_of(1))

    def all_sent(to):
        part = gathered.at[pl.ds(0, count - 1)]
        return remote(part, part, to, two_recv.at[0], row=peer_of(1))

    def all_side():
        part = taper_all.at[pl.ds(0, count - 1), pl.ds(0, share), pl.ds(0, lanes)]
        return remote(part, part, side_send.at[0], side_recv.at[0], row=peer_of(1))

    def all_lev(blocks):
        part = taper_all.at[pl.ds(0, blocks), pl.ds(0, share)]
        return remote(part, part, lev_send.at[0], lev_recv.at[0], lev=levs - 1 - lev_at)

    corners = inner > 1 and levs > 1 and outer > 1
    at_end = (line_at == 0) | (line_at == outer - 1)
    far = jnp.where(line_at == 0, outer - 1, 0) * inner + inner - 1

    def corner(lev):
        part = piece(far, lev, side_at)
        return remote(part, part, lev_send.at[1], lev_recv.at[1], lev=levs - 1 - lev_at)

    def opposite(at):
        part = piece(far, levs - 1 - lev_at, at)
        return remote(part, part, first_send.at[1], first_recv.at[1], row=other)

    def each_lev(action):
        if corners:
            pl.when(at_end)(lambda: action(all_lev(count - 2)))
            pl.when(jnp.logical_not(at_end))(lambda: action(all_lev(count - 1)))
        else:
            action(all_lev(count - 1))

    def pert_copy(peer, slot):
        return remote(
            pert.at[:, :, :, :, own_columns(peer)], pert_all.at[slot], pert_send.at[peer],
            pert_recv.at[slot], mem=peer,
        )

    def piece(origin, lev, side):
        return taper_all.at[
            origin,
            pl.ds(pl.multiple_of(lev * share, share), share),
            pl.ds(pl.multiple_of(side * lanes, lanes), lanes),
        ]

    other = line_at * inner + (inner - 1 - side_at)

    def first(origin, side):
        part = piece(origin, lev_at, side)
        return remote(part, part, first_send.at[0], first_recv.at[0], row=other)

    def side(origin, at):
        part = piece(origin, lev_at, at)
        return remote(part, part, side_send.at[0], side_recv.at[origin], row=other)

    def line(way, hop, turn, sending):
        back = hop if sending else hop + 1
        from_line = line_at - back if way == 0 else line_at + back
        to_line = line_at + 1 if way == 0 else line_at - 1
        origin = from_line * inner + (side_at if turn == 0 else inner - 1 - side_at)
        there = from_line >= 0 if way == 0 else from_line <= outer - 1
        if sending:
            there = there & (to_line <= outer - 1 if way == 0 else to_line >= 0)

        def copy():
            part = piece(origin, lev_at, side_at)
            return remote(
                part, part, line_send.at[way, hop, turn], line_recv.at[way, hop, turn],
                row=to_line * inner + side_at,
            )

        return origin, there, copy

    def across(there, origin, at):
        def copy():
            part = piece(origin, lev_at, at)
            return remote(part, part, lev_send.at[0], lev_recv.at[0], lev=levs - 1 - lev_at)

        if levs > 1:
            start(there, copy)

    def along_line(hop, turn):
        if outer == 1:
            return
        for way in range(2):
            _, there, copy = line(way, hop, turn, True)
            send(there, copy)

    def one_chunk(turn, half=None):
        level = level_of(turn)
        cut = (len(offsets) + 1) // 2
        part = offsets if half is None else offsets[:cut] if half == 0 else offsets[cut:]
        for by in part:
            start(True, lambda by=by: one(peer_of(by), me, level))

    def row_step(turn):
        level = level_of(turn)
        if count > 1:
            all_one(level).wait_recv()
        whole = row_all[...].reshape(count * rows, count * rows)
        for member in range(members):
            tapered = jnp.dot(
                whole, gathered[:, level, member].reshape(count * rows, depth),
                preferred_element_type=jnp.float32,
            )
            staged[:, level, member] = tapered.astype(jnp.bfloat16).reshape(count, rows, depth)
        for by in offsets:
            start(True, lambda by=by: two(peer_of(by), me, level))
        for member in range(members):
            halves[level, me, mem_at, member] = staged[me, level, member]

    def set_factors():
        row_at = lax.broadcasted_iota(jnp.int32, (rows, width), 0)
        column_at = lax.broadcasted_iota(jnp.int32, (rows, width), 1)
        for turn in range(levels):
            level = level_of(turn)
            centre = jnp.ones((rows, width), jnp.float32)
            for at in range(3):
                speed = courant[at, level]
                ahead, back = jnp.maximum(speed, 0.0), -jnp.minimum(speed, 0.0)
                centre = centre - ahead - back
                if at == 0:
                    ahead, back = jnp.where(lev_at > 0, ahead, back), jnp.where(lev_at > 0, back, ahead)
                if at == 1:
                    ahead = jnp.where(row_at == 0, 0.0, ahead)
                    back = jnp.where(row_at == rows - 1, 0.0, back)
                if at == 2:
                    ahead = jnp.where(column_at == 0, 0.0, ahead)
                    back = jnp.where(column_at == width - 1, 0.0, back)
                factors[1 + 2 * at, turn] = ahead
                factors[2 + 2 * at, turn] = back
            factors[0, turn] = centre

    neighbours = []
    if count > 1:
        neighbours += [("row", 0, me > 0, me - 1), ("row", 1, me < count - 1, me + 1)]
    if mems > 1:
        neighbours += [("mem", 0, mem_at > 0, mem_at - 1), ("mem", 1, mem_at < mems - 1, mem_at + 1)]

    def part_of(turn):
        return min(turn, 1)

    def turns_of(part):
        return range(0, 1) if part == 0 else range(1, levels)

    parts = 1 if levels == 1 else 2

    def edge_copy(step, kind, part, axis, at, target, arriving):
        at_kind, turns = (kind, pl.ds(0, 1)) if part == 0 else (pl.ds(0, kinds), pl.ds(1, levels - 1))
        landed, slot = at if arriving else 1 - at, kind if part == 0 else kinds
        if axis == "row":
            source = row_edge.at[step, at, at_kind, turns]
            landing = row_halo.at[step, landed, at_kind, turns]
            to, there = edge_send.at[step, at], edge_recv.at[step % 2, landed, slot]
        else:
            source = state.at[step, at_kind, turns, :, pl.ds(0 if at == 0 else width - 128, 128)]
            landing = column_halo.at[step, landed, at_kind, turns]
            place = column_recv.shape[1]
            to, there = column_send.at[step, at % place], column_recv.at[step % 2, landed % place, slot]
        return remote(landing if arriving else source, landing, to, there, **{axis: target})

    def level_copy(step, kind):
        return remote(
            level_send.at[step, kind], level_halo.at[step, kind], up_send.at[step],
            up_recv.at[step % 2, kind], lev=levs - 1 - lev_at,
        )

    def send_edges(step, kind, part):
        for axis, at, there, target in neighbours:

            @pl.when(there)
            def _():
                if axis == "row":
                    for variable in [kind] if part == 0 else range(kinds):
                        for turn in turns_of(part):
                            row_edge[step, at, variable, turn] = state[
                                step, variable, turn, pl.ds(0 if at == 0 else rows - 1, 1)
                            ]
                edge_copy(step, kind, part, axis, at, target, False).start()

    def settle_step(step):
        if levs > 1:
            remote(
                level_send.at[step], level_send.at[step], up_send.at[step], up_recv.at[step % 2, 0],
                lev=levs - 1 - lev_at,
            ).wait_send()
        for axis, at, there, target in neighbours:

            @pl.when(there)
            def _():
                part = (row_edge if axis == "row" else column_halo).at[step, at]
                place = at % column_recv.shape[1]
                to = edge_send.at[step, at] if axis == "row" else column_send.at[step, place]
                remote(part, part, to, edge_recv.at[0, 0, 0], **{axis: target}).wait_send()

    def inside(step, kind, turn, target):
        here = state[step, kind, turn]
        new = here * factors[0, turn]
        new = new + factors[3, turn] * pltpu.roll(here, 1, 0)
        new = new + factors[4, turn] * pltpu.roll(here, rows - 1, 0)
        new = new + factors[5, turn] * pltpu.roll(here, 1, 1)
        new = new + factors[6, turn] * pltpu.roll(here, width - 1, 1)
        if turn > 0:
            new = new + factors[1, turn] * state[step, kind, turn - 1]
        if turn < levels - 1:
            new = new + factors[2, turn] * state[step, kind, turn + 1]
        if kind == 2:
            level = level_of(turn)
            new = new - (
                state[step, 0, turn] * slope[0, level] + state[step, 1, turn] * slope[1, level]
            )
        target[...] = new

    def take_edges(step, kind, part, view):
        lane_at = lax.broadcasted_iota(jnp.int32, (rows, 128), 1)
        for axis, at, there, target in neighbours:

            @pl.when(there)
            def _():
                edge_copy(step, kind, part, axis, at, target, True).wait_recv()
                whole = [kind] if part == 0 else range(kinds)
                for kind_at, turn in [(k, t) for k in whole for t in turns_of(part)]:
                    level, new = level_of(turn), view(kind_at, turn)
                    if axis == "row":
                        edge = pl.ds(0 if at == 0 else rows - 1, 1)
                        speed = courant[1, level, edge]
                        speed = -jnp.minimum(speed, 0.0) if at else jnp.maximum(speed, 0.0)
                        new[edge] = new[edge] + speed * row_halo[step, at, kind_at, turn]
                    else:
                        columns_at = pl.ds(width - 128 if at else 0, 128)
                        speed = courant[2, level, :, columns_at]
                        speed = -jnp.minimum(speed, 0.0) if at else jnp.maximum(speed, 0.0)
                        beside = pltpu.roll(
                            column_halo[step, at, kind_at, turn], 127 if at else 1, 1
                        )
                        new[:, columns_at] = new[:, columns_at] + jnp.where(
                            lane_at == (127 if at else 0), speed * beside, 0.0
                        )

    def one_step(step, view, last):
        for kind in range(kinds):
            inside(step, kind, 0, view(kind, 0))
        for kind in range(kinds):
            for turn in turns_of(1):
                inside(step, kind, turn, view(kind, turn))
            take_edges(step, kind, 0, view)
            if levs > 1:
                level_copy(step, kind).wait_recv()
                new = view(kind, 0)
                whole = new[...] + factors[1, 0] * level_halo[step, kind].astype(jnp.float32)
                new[...] = whole
                if not last:
                    level_send[step + 1, kind] = whole.astype(level_send.dtype)
                    level_copy(step + 1, kind).start()
            if not last:
                send_edges(step + 1, kind, 0)
        if parts > 1:
            take_edges(step, 0, 1, view)
            if not last:
                send_edges(step + 1, 0, 1)
        settle_step(step)

    barrier = pltpu.get_barrier_semaphore()
    for axis, here, size in (("row", me, count), ("mem", mem_at, mems), ("lev", lev_at, levs)):

        @pl.loop(1, size)
        def _(shift):
            pl.semaphore_signal(
                barrier, inc=1, device_id={axis: (here + shift) % size}, device_id_type=MESH
            )

    fetches = [
        pltpu.make_async_copy(taper.at[:, own_columns(mem_at)], taper_all.at[me], own_sem.at[0]),
        pltpu.make_async_copy(control, own, own_sem.at[1]),
        pltpu.make_async_copy(row_part, row_all.at[me], own_sem.at[2]),
        pltpu.make_async_copy(
            pert.at[:, :, :, :, own_columns(mem_at)], pert_all.at[mem_at], own_sem.at[3]
        ),
    ]
    late = [
        pltpu.make_async_copy(courant_in, courant, own_sem.at[4 + levels]),
        pltpu.make_async_copy(slope_in, slope, own_sem.at[5 + levels]),
    ]
    for level in range(levels):
        fetches.append(
            pltpu.make_async_copy(
                block(control, me, level), gathered.at[me, level], own_sem.at[4 + level]
            )
        )
    for fetch in fetches + late:
        fetch.start()
    for fetch in fetches[:3]:
        fetch.wait()
    pl.semaphore_wait(barrier, count + mems + levs - 3)

    if inner > 1:
        send(True, lambda: first(me, inner - 1 - side_at))
    along_line(0, 0)
    if inner > 1:
        start(True, lambda: side(me, side_at))
    for by in offsets:
        start(True, lambda by=by: row(peer_of(by), me))
    one_chunk(0)
    for shift in range(1, mems):
        send(True, lambda shift=shift: pert_copy((mem_at + shift) % mems, mem_at))
    for fetch in fetches[3:] + late:
        fetch.wait()
    set_factors()

    def hop_step(hop, turn):
        for way in range(2):
            origin, there, copy = line(way, hop, turn, False)

            def arrived(copy=copy):
                copy().wait_recv()

            when(there, arrived)
            if hop + 1 < outer - 1:
                _, onwards, relay = line(way, hop + 1, turn, True)
                send(onwards, relay)
            if inner > 1:
                start(there, lambda origin=origin: side(origin, side_at))
            if corners and hop == outer - 2:
                across(there & (side_at == turn), origin, side_at)
                start(there & (side_at != turn), lambda: corner(lev_at))
            else:
                across(there, origin, side_at)

    def side_step(hop):
        for turn in range(inner):
            for way in range(2):
                origin, there, _ = line(way, hop, turn, False)
                if inner > 1:

                    def arrived(origin=origin):
                        side(origin, inner - 1 - side_at).wait_recv()

                    when(there, arrived)
                    if corners and hop == outer - 2:
                        across(there & (side_at == turn), origin, inner - 1 - side_at)
                    else:
                        across(there, origin, inner - 1 - side_at)
        if corners and hop == outer - 2:

            @pl.when(at_end)
            def _():
                corner(levs - 1 - lev_at).wait_recv()
                opposite(side_at).start()

    span = min(width, 256)

    def product_step(turn):
        level = level_of(turn)
        for shift in range(1, mems):
            peer = (mem_at + shift) % mems

            onward(peer, level, peer).wait_recv()

        for start in range(0, width, span):
            total = jnp.zeros((mems * members * rows, span), jnp.float32)
            for slot in range(count):
                total = total + jnp.dot(
                    halves[level, slot].reshape(mems * members * rows, depth),
                    taper_all[slot, :, pl.ds(start, span)],
                    preferred_element_type=jnp.float32,
                )
            for kind in range(kinds):
                weighted = jnp.zeros((rows, span), jnp.float32)
                for mem in range(mems):
                    for member in range(members):
                        at = (mem * members + member) * rows
                        weighted = weighted + pert_all[
                            mem, kind, member, level, :, pl.ds(start, span)
                        ].astype(jnp.float32) * total[at : at + rows]
                state[0, kind, turn, :, pl.ds(start, span)] = weighted
                if turn == 0 and levs > 1:
                    level_send[0, kind, :, pl.ds(start, span)] = weighted.astype(level_send.dtype)
        if turn == 0:
            for kind in range(kinds):
                if levs > 1:
                    level_copy(0, kind).start()
                send_edges(0, kind, 0)

    def first_step():
        if inner > 1:
            first(other, side_at).wait_recv()
            along_line(0, 1)
            across(True, other, side_at)

    def other_step():
        if inner > 1:
            side(other, inner - 1 - side_at).wait_recv()
            across(True, other, inner - 1 - side_at)

    def whole_row():
        if count > 1:
            all_row().wait_recv()

    def back_step(turn):
        level = level_of(turn)
        if count > 1:
            all_two(level).wait_recv()
        for shift in range(1, mems):
            onward((mem_at + shift) % mems, level, mem_at).start()

    def taper_whole():
        for there, copy in early:
            when(there, lambda copy=copy: copy().wait_send())
        if count > 1:
            all_row().wait_send()
            all_sent(one_send.at[0]).wait_send()
            if inner > 1:
                all_side().wait_send()
            if levs > 1:
                each_lev(lambda copy: copy.wait_recv())
            if corners:

                @pl.when(at_end)
                def _():
                    opposite(inner - 1 - side_at).wait_recv()
        for shift in range(1, mems):
            peer = (mem_at + shift) % mems
            pert_copy(peer, peer).wait_recv()

    def settle():
        if count > 1:
            all_sent(two_send.at[0]).wait_send()
            if levs > 1:
                each_lev(lambda copy: copy.wait_send())
            if corners:

                @pl.when(at_end)
                def _():
                    corner(lev_at).wait_send()
                    opposite(side_at).wait_send()
        for level in range(levels):
            for shift in range(1, mems):
                onward((mem_at + shift) % mems, level, mem_at).wait_send()

    first_step()
    chunks = [(turn, half) for turn in range(1, levels) for half in range(2)]
    turns_left = list(range(levels))

    def next_chunk():
        if chunks:
            one_chunk(*chunks.pop(0))

    def next_row():
        if turns_left:
            turn = turns_left.pop(0)
            while chunks and chunks[0][0] <= turn:
                next_chunk()
            if turn == 0:
                whole_row()
            row_step(turn)

    for hop in range(outer - 1):
        hop_step(hop, 0)
        if hop == 0:
            next_chunk()
            other_step()
        if hop == 1:
            side_step(0)
        for turn in range(1, inner):
            hop_step(hop, turn)
        if hop == 0:
            next_chunk()
            if outer == 2:
                side_step(0)
        elif hop < outer - 2:
            next_chunk()
            side_step(hop)
            next_chunk()
            next_row()
            next_row()
        else:
            next_row()
            side_step(hop)
    if outer == 1:
        other_step()
    for _ in range(levels):
        next_row()
    for turn in range(levels - 1):
        back_step(turn)
    taper_whole()
    for turn in range(levels - 1):
        product_step(turn)
    back_step(levels - 1)
    product_step(levels - 1)
    if parts > 1:
        send_edges(0, 0, 1)
    settle()

    @pl.loop(0, STEPS - 1)
    def _(step):
        one_step(step, lambda kind, turn: state.at[step + 1, kind, turn], False)

    one_step(STEPS - 1, lambda kind, turn: out.at[kind, level_of(turn)], True)


def on_device(
    control_fields, perturbations, column_taper, row_taper, courant_numbers, tracer_slope
):
    members, levels, rows, columns = control_fields.shape
    kinds = perturbations.shape[0]
    count, mems, levs = (lax.axis_size(axis) for axis in ("row", "mem", "lev"))
    depth, width = columns // count, columns // mems
    if depth % 128:
        control_fields = control_fields.reshape(members, levels, rows, count, depth)
        control_fields = control_fields.transpose(3, 0, 1, 2, 4)
    low, full, dma = jnp.bfloat16, jnp.float32, pltpu.SemaphoreType.DMA
    inner = 2 if count % 2 == 0 else 1
    sides, hops = max(1, min(2, mems - 1)), max(1, count // inner - 1)
    semaphores = [dma((1,)), dma((levels,)), dma((1,)), dma((1,)), dma((1,)), dma((levels,))]
    semaphores += [dma((mems, levels))] * 2 + [dma((mems,))] * 2 + [dma((2,))] * 2
    semaphores += [dma((2, hops, inner))] * 2 + [dma((1,)), dma((count,)), dma((2,)), dma((2,))]
    semaphores += [dma((STEPS,)), dma((2, kinds)), dma((STEPS, 2)), dma((2, 2, kinds + 1))]
    semaphores += [dma((STEPS, sides)), dma((2, sides, kinds + 1))]
    return pl.pallas_call(
        kernel,
        out_shape=jax.ShapeDtypeStruct((kinds, levels, rows, width), full),
        in_specs=[pl.BlockSpec(memory_space=pltpu.HBM)] * 6,
        out_specs=pl.BlockSpec(memory_space=pltpu.VMEM),
        scratch_shapes=[
            pltpu.VMEM(control_fields.shape, low),
            pltpu.VMEM((count, levels, members, rows, depth), low),
            pltpu.VMEM((count, rows, count * rows), low),
            pltpu.VMEM((count, levels, members, rows, depth), low),
            pltpu.VMEM((levels, count, mems, members, rows, depth), low),
            pltpu.VMEM((count, depth, width), low),
            pltpu.VMEM((mems, kinds, members, levels, rows, width), low),
            pltpu.VMEM(courant_numbers.shape, full),
            pltpu.VMEM(tracer_slope.shape, full),
            pltpu.VMEM((STEPS, kinds, levels, rows, width), full),
            pltpu.VMEM((7, levels, rows, width), full),
            pltpu.VMEM((STEPS, kinds, rows, width), low),
            pltpu.VMEM((STEPS, kinds, rows, width), low),
            pltpu.VMEM((STEPS, 2, kinds, levels, 1, width), full),
            pltpu.VMEM((STEPS, 2, kinds, levels, 1, width), full),
            pltpu.VMEM((STEPS, 2, kinds, levels, rows, 128), full),
            *semaphores,
            dma((6 + levels,)),
        ],
        compiler_params=pltpu.CompilerParams(
            collective_id=0, has_side_effects=True, vmem_limit_bytes=44 << 20
        ),
        name="increment",
    )(
        *(
            pltpu.with_memory_space_constraint(operand, pltpu.HBM)
            for operand in (
                control_fields, perturbations, column_taper, row_taper, courant_numbers, tracer_slope
            )
        )
    )


def solution(mesh):
    assert mesh.shape["lev"] <= 2
    placed = (
        P("mem", "lev", "row", None),
        P(None, "mem", "lev", "row", None),
        P("row", None),
        P("row", None),
        P(None, "lev", "row", "mem"),
        P(None, "lev", "row", "mem"),
    )
    return jax.shard_map(
        on_device,
        mesh=mesh,
        in_specs=placed,
        out_specs=P(None, "lev", "row", "mem"),
        check_vma=False,
    )
```
